128 devices in a mesh: dp: 8 (over x_lo, y), tensor: 16 (over x_hi, z, core).
Axes of the slice: x: 4 (x_hi: 2, x_lo: 2; x = x_hi * 2 + x_lo), y: 4, z: 4, core: 2. Of those that a mesh axis runs over, the one named last changes fastest.
Arguments:
- activations: bfloat16 [12288, 8192], P('dp', 'tensor'), may hold values from -6 to 6
- deltas: bfloat16 [12288, 28672], P('dp', 'tensor'), may hold values from -6 to 6
- query_in: bfloat16 [8192, 1024], P('tensor', 'dp'), may hold values from -0.0625 to 0.0625
- query_out: bfloat16 [28672, 1024], P('tensor', 'dp'), may hold values from -0.03125 to 0.03125
- doc_ids: int32 [12288], P('dp'), may hold values from 0 to 63, never falling along the last dimension, each value on 1 to 384 neighbouring positions
Outputs:
- scores: float32 [12288, 32], P('dp')
- doc_scores: float32 [64, 32], replicated
The draws below stay inside these ranges and needn't reach their ends.
Inputs may be any that keep to these rules, and one draw needn't show every extreme that they name: doc_ids never falls along the tokens; every document owns 1 to 384 tokens, and one owns exactly 384.
All inputs are finite; a program needn't handle non-finite values.
Results may differ from the reference program's by a relative error of at most 0.0003.
Values may be sent and summed in bfloat16 or wider, within the bound.
A program may use at most 128 MiB of HBM per device.

```python
import math
import jax
import jax.numpy as jnp
import numpy as np

D = 8192
FF = 28672
RANK = 32
TOKENS = 12288
NQUERIES = 32
DOCS = 64
MOST = 384


def levels(stream_key, dims, split, low, high):
    factor_of = 1.0
    for dim, blocks in split:
        heights = jax.random.uniform(jax.random.fold_in(jax.random.fold_in(stream_key, 6), dim), (blocks,), jnp.float32, low / len(split), high / len(split))
        factor_of = factor_of * jnp.repeat(jnp.exp(heights), dims[dim] // blocks).reshape((-1,) + (1,) * (len(dims) - 1 - dim))
    return factor_of


def split_up(amount, total, bound, lean):
    portions = [(1 << 20) // math.isqrt(grade ** lean) + 1 for grade in range(2, amount + 1)]
    rest, holding = total - bound - (amount - 1), [1] * (amount - 1)
    while rest > 0:
        candidates = [i for i in range(amount - 1) if holding[i] < bound]
        mass, left = sum([portions[i] for i in candidates]), rest
        for i in candidates:
            addition = min(bound - holding[i], max(1, left * portions[i] // mass), rest)
            holding[i] = holding[i] + addition
            rest = rest - addition
    return np.array([bound] + holding)


def ragged(rng, number_of, total, reach, lean):
    if number_of == 2:
        one = jax.random.randint(rng, (), max(1, total - reach), min(reach, total - 1) + 1)
        return jnp.stack([one, total - one])
    tallies = jnp.asarray(split_up(number_of, total, reach, lean), jnp.int32)
    couples = (number_of - 1) // 2
    giver, receiver = tallies[1:1 + 2 * couples:2], tallies[2:2 + 2 * couples:2]
    slack = jnp.minimum(giver - 1, reach - receiver)
    moved = jax.random.randint(jax.random.fold_in(rng, 1), (couples,), 0, 1 << 20) % (slack + 1)
    tallies = tallies.at[1:1 + 2 * couples:2].set(giver - moved).at[2:2 + 2 * couples:2].set(receiver + moved)
    return tallies[jax.random.permutation(jax.random.fold_in(rng, 2), number_of)]


def normal_values(stream_key, extent, width, bound, cuts=(), kind=jnp.bfloat16):
    array = width * jax.random.normal(stream_key, extent, jnp.float32)
    if cuts:
        array = array * levels(stream_key, extent, cuts, -0.22, 0.18)
    return jnp.clip(array, -bound, bound).astype(kind)


def setup_inputs(seed: int = 0) -> dict:
    splits = jax.random.split(jax.random.key(seed), 6)
    activations = normal_values(splits[0], (TOKENS, D), 1.0, 6.0, ((0, 8), (1, 16)))
    deltas = normal_values(splits[1], (TOKENS, FF), 1.0, 6.0, ((0, 8), (1, 16)))
    query_in = normal_values(splits[2], (D, NQUERIES * RANK), D ** -0.5, 0.0625, ((0, 16), (1, 8)))
    query_out = normal_values(splits[3], (FF, NQUERIES * RANK), FF ** -0.5, 0.03125, ((0, 16), (1, 8)))
    doc_ids = jnp.searchsorted(jnp.cumsum(ragged(splits[4], DOCS, TOKENS, MOST, 1)), jnp.arange(TOKENS), side="right").astype(jnp.int32)
    return dict(activations=activations, deltas=deltas, query_in=query_in, query_out=query_out, doc_ids=doc_ids)


def reference(activations, deltas, query_in, query_out, doc_ids):
    proj_in = jnp.dot(activations, query_in, preferred_element_type=jnp.float32)
    proj_out = jnp.dot(deltas, query_out, preferred_element_type=jnp.float32)
    products = (proj_in * proj_out).reshape(TOKENS, NQUERIES, RANK)
    scores = jnp.sum(products, axis=2) * jnp.float32(RANK ** -0.5)
    sums = jax.ops.segment_sum(scores, doc_ids, DOCS)
    counts = jax.ops.segment_sum(jnp.ones((TOKENS,), jnp.float32), doc_ids, DOCS)
    doc_scores = sums / counts[:, None]
    return scores, doc_scores
```

```python
import jax
import jax.numpy as jnp
from jax import lax
from jax.experimental import pallas as pl
from jax.experimental.pallas import tpu as pltpu
from jax.sharding import PartitionSpec as P

RANK = 32
MESH = pl.DeviceIdType.MESH
F32 = jnp.float32
HIGHEST = lax.Precision.HIGHEST

ROWS = 1536
HALF = ROWS // 2
ZCH = HALF // 4
CH = ZCH // 2
KIN = 512
KOUT = 1792
K = KIN + KOUT
KH = K // 2
NB = 8
TM = 256
D2D, HA, HB, RMA, RMB, RPA, RPB, XH = range(8)


def nt(a, b):
    return lax.dot_general(
        a, b, (((1,), (1,)), ((), ())), precision=HIGHEST, preferred_element_type=F32
    )


def kernel(
    act, dl, qi, qo, ids, scores_out, docs_out,
    a_in, a_out, q, p, dbuf, h, rm, rp, xb, acc, msg, g, dpb,
    lsem, qs, qr, rs, rr, gs, gr, ds_, dr,
):
    dp = lax.axis_index("dp")
    t = lax.axis_index("tensor")
    xl, y = dp // 4, dp % 4
    hx, z, c = t // 8, (t // 2) % 4, t % 2

    x_lo = {"dp": (dp + 4) % 8, "tensor": t}
    y_up = {"dp": xl * 4 + (y + 1) % 4, "tensor": t}
    y_dn = {"dp": xl * 4 + (y + 3) % 4, "tensor": t}
    x_hi = {"dp": dp, "tensor": (t + 8) % 16}
    z_up = {"dp": dp, "tensor": hx * 8 + ((z + 1) % 4) * 2 + c}
    z_dn = {"dp": dp, "tensor": hx * 8 + ((z + 3) % 4) * 2 + c}
    mate = {"dp": dp, "tensor": hx * 8 + z * 2 + 1 - c}

    loads = [
        pltpu.make_async_copy(qi, q.at[0, pl.ds(0, KIN)], lsem.at[0]),
        pltpu.make_async_copy(qo, q.at[0, pl.ds(KIN, KOUT)], lsem.at[1]),
        pltpu.make_async_copy(act, a_in, lsem.at[2]),
        pltpu.make_async_copy(dl, a_out, lsem.at[3]),
    ]
    for cp in loads:
        cp.start()

    barrier = pltpu.get_barrier_semaphore()
    for k in range(1, 16):
        pl.semaphore_signal(
            barrier, inc=1, device_id={"dp": dp, "tensor": (t + k) % 16}, device_id_type=MESH
        )
    for k in range(1, 8):
        pl.semaphore_signal(
            barrier, inc=1, device_id={"dp": (dp + k) % 8, "tensor": t}, device_id_type=MESH
        )
    pl.semaphore_wait(barrier, 22)

    sent = []

    def send(src, dst, ss, rsem, to):
        cp = pltpu.make_async_remote_copy(
            src_ref=src, dst_ref=dst, send_sem=ss, recv_sem=rsem,
            device_id=to, device_id_type=MESH,
        )
        cp.start()
        sent.append(cp)
        return cp

    lo, hi, full = pl.ds(0, KH), pl.ds(KH, KH), pl.ds(0, K)

    def qsend(n, src, dst, rows, to):
        return send(q.at[src, rows], q.at[dst, rows], qs.at[n], qr.at[n], to)

    loads[0].wait()
    loads[1].wait()
    q1 = qsend(0, 0, 1, full, x_lo)
    q3 = qsend(1, 0, 3, full, y_up)
    q2 = qsend(2, 0, 2, full, y_dn)
    loads[2].wait()
    loads[3].wait()

    moves = {}

    def rsend(b, role, src, dst, to):
        moves[b, role] = send(src, dst, rs.at[role, b], rr.at[role, b], to)

    own, other = c * HALF, (1 - c) * HALF

    def zrows(dz, part=0, n=CH):
        at = own + ((z + dz) % 4) * ZCH + part * CH
        return pl.ds(pl.multiple_of(at, CH), n)

    def mm(b):
        for base in (other, own):

            def tile(i, carry, base=base):
                rows = pl.ds(pl.multiple_of(base + i * TM, TM), TM)
                p[b, rows, pl.ds(0, 128)] = jnp.dot(
                    a_in[rows, :], q[b, pl.ds(0, KIN), :], preferred_element_type=F32
                )
                p[b, rows, pl.ds(128, 128)] = jnp.dot(
                    a_out[rows, :], q[b, pl.ds(KIN, KOUT), :], preferred_element_type=F32
                )
                return carry

            lax.fori_loop(0, HALF // TM, tile, 0)
            if base is other:
                rsend(b, D2D, p.at[b, pl.ds(pl.multiple_of(other, HALF), HALF)], dbuf.at[b], mate)

    def step1(b):
        moves[b, D2D].wait_recv()
        rows = pl.ds(pl.multiple_of(own, HALF), HALF)
        p[b, rows, :] += dbuf[b]
        rsend(b, HA, p.at[b, zrows(2, 0)], h.at[b, 0], z_up)
        rsend(b, HB, p.at[b, zrows(2, 1)], h.at[b, 1], z_dn)
        rsend(b, RMB, p.at[b, zrows(1, 1)], rm.at[b, 1], z_up)
        rsend(b, RPA, p.at[b, zrows(3, 0)], rp.at[b, 0], z_dn)

    def step2(b):
        moves[b, HA].wait_recv()
        p[b, zrows(1, 0), :] += h[b, 0]
        rsend(b, RMA, p.at[b, zrows(1, 0)], rm.at[b, 0], z_up)
        moves[b, HB].wait_recv()
        p[b, zrows(3, 1), :] += h[b, 1]
        rsend(b, RPB, p.at[b, zrows(3, 1)], rp.at[b, 1], z_dn)

    def zsum(b, part):
        p[b, zrows(0, part), :] += rm[b, part] + rp[b, part]

    def step3(b):
        for role in (RMB, RPA, RMA, RPB):
            moves[b, role].wait_recv()
        p[b, zrows(0, 1 - hx), :] += rm[b, 1 - hx] + rp[b, 1 - hx]
        rsend(b, XH, p.at[b, zrows(0, 1 - hx)], xb.at[b], x_hi)
        p[b, zrows(0, hx), :] += rm[b, hx] + rp[b, hx]

    source = [
        dp, (dp + 4) % 8,
        xl * 4 + (y + 1) % 4, xl * 4 + (y + 3) % 4, xl * 4 + (y + 2) % 4,
        (1 - xl) * 4 + (y + 1) % 4, (1 - xl) * 4 + (y + 3) % 4, (1 - xl) * 4 + (y + 2) % 4,
    ]

    def step4(b):
        moves[b, XH].wait_recv()
        total = p[b, zrows(0, hx), :] + xb[b]
        prod = total[:, :128] * total[:, 128:]
        prod = jnp.concatenate([prod, jnp.zeros((128 - CH, 128), F32)], axis=0)
        row = lax.broadcasted_iota(jnp.int32, (32, 128), 0)
        col = lax.broadcasted_iota(jnp.int32, (32, 128), 1)
        pick = (row == source[b] * 4 + col // RANK).astype(F32)
        acc[...] += nt(pick, prod)

    acc[...] = jnp.zeros_like(acc)
    mm(0)
    step1(0)
    step2(0)
    step3(0)

    q3.wait_recv()
    q4a = qsend(3, 3, 4, lo, y_up)
    q2.wait_recv()
    q4b = qsend(4, 2, 4, hi, y_dn)
    q1.wait_recv()
    q6 = qsend(5, 1, 6, full, y_up)
    q5 = qsend(6, 1, 5, full, y_dn)
    mm(1)
    mm(2)
    step1(1)
    mm(3)
    step1(2)
    step2(1)
    step1(3)
    step2(2)
    step3(1)
    q4a.wait_recv()
    q4b.wait_recv()
    mm(4)
    step4(0)
    step1(4)
    step2(3)
    step3(2)
    step4(1)
    step2(4)
    step3(3)
    q6.wait_recv()
    q7a = qsend(7, 6, 7, lo, y_up)
    q5.wait_recv()
    q7b = qsend(8, 5, 7, hi, y_dn)
    mm(5)
    mm(6)
    step1(5)
    step3(4)
    step4(2)
    step1(6)
    step2(5)
    q7a.wait_recv()
    q7b.wait_recv()
    mm(7)
    step2(6)
    step1(7)
    step3(5)
    step4(3)
    step2(7)
    step3(6)
    step4(4)
    step3(7)
    step4(5)
    step4(6)
    step4(7)

    slot = c * 8 + z * 2 + hx
    mine = acc[...] * F32(RANK ** -0.5)
    seen = ids[pl.ds(slot, 1), :]
    doc = lax.broadcasted_iota(jnp.int32, (128, 128), 0)
    sums = nt(mine, (doc == seen).astype(F32))
    counts = nt(jnp.ones((32, 128), F32), (doc - 64 == seen).astype(F32))
    msg[pl.ds(0, 32), :] = mine
    msg[pl.ds(32, 32), :] = sums + counts
    g[slot] = msg[...]
    got = []
    for k in range(1, 16):
        to = {"dp": dp, "tensor": (t + k) % 16}
        got.append(send(msg, g.at[slot], gs.at[k - 1], gr.at[k - 1], to))
    for cp in got:
        cp.wait_recv()
    part = g[0, pl.ds(32, 32), :]
    for m in range(1, 16):
        part = part + g[m, pl.ds(32, 32), :]
    dpb[dp] = part
    got = []
    for k in range(1, 8):
        to = {"dp": (dp + k) % 8, "tensor": t}
        got.append(send(dpb.at[dp], dpb.at[dp], ds_.at[k - 1], dr.at[k - 1], to))
    scores_out[...] = jnp.concatenate([g[m, pl.ds(0, 32), :][:, :CH] for m in range(16)], axis=1)
    for cp in got:
        cp.wait_recv()
    whole = dpb[0]
    for m in range(1, 8):
        whole = whole + dpb[m]
    docs_out[...] = (whole / pltpu.roll(whole, 64, 1))[:, :64]
    for cp in sent:
        cp.wait_send()


def body(activations, deltas, query_in, query_out, doc_ids):
    ids = jnp.pad(doc_ids.reshape(16, CH), ((0, 0), (0, 128 - CH)), constant_values=-1000)
    any_ = pl.BlockSpec(memory_space=pl.ANY)
    vmem = pl.BlockSpec(memory_space=pltpu.VMEM)
    dma = pltpu.SemaphoreType.DMA
    scores, docs = pl.pallas_call(
        kernel,
        out_shape=(
            jax.ShapeDtypeStruct((32, ROWS), F32),
            jax.ShapeDtypeStruct((32, 64), F32),
        ),
        in_specs=[any_, any_, any_, any_, vmem],
        out_specs=(vmem, vmem),
        scratch_shapes=[
            pltpu.VMEM((ROWS, KIN), jnp.bfloat16),
            pltpu.VMEM((ROWS, KOUT), jnp.bfloat16),
            pltpu.VMEM((NB, K, 128), jnp.bfloat16),
            pltpu.VMEM((NB, ROWS, 256), F32),
            pltpu.VMEM((NB, HALF, 256), F32),
            pltpu.VMEM((NB, 2, CH, 256), F32),
            pltpu.VMEM((NB, 2, CH, 256), F32),
            pltpu.VMEM((NB, 2, CH, 256), F32),
            pltpu.VMEM((NB, CH, 256), F32),
            pltpu.VMEM((32, 128), F32),
            pltpu.VMEM((64, 128), F32),
            pltpu.VMEM((16, 64, 128), F32),
            pltpu.VMEM((8, 32, 128), F32),
            dma((4,)), dma((9,)), dma((9,)), dma((8, NB)), dma((8, NB)),
            dma((15,)), dma((15,)), dma((7,)), dma((7,)),
        ],
        compiler_params=pltpu.CompilerParams(
            collective_id=0, has_side_effects=True, vmem_limit_bytes=60 * 1024 * 1024
        ),
    )(activations, deltas, query_in, query_out, ids)
    return scores.T, docs.T


def solution(mesh):
    return jax.shard_map(
        body,
        mesh=mesh,
        in_specs=(
            P("dp", "tensor"),
            P("dp", "tensor"),
            P("tensor", "dp"),
            P("tensor", "dp"),
            P("dp"),
        ),
        out_specs=(P("dp", None), P()),
        check_vma=False,
    )
```

```python
import jax
import jax.numpy as jnp
from jax import lax
from jax.experimental import pallas as pl
from jax.experimental.pallas import tpu as pltpu
from jax.sharding import PartitionSpec as P

RANK = 32
MESH = pl.DeviceIdType.MESH
F32 = jnp.float32
HIGHEST = lax.Precision.HIGHEST

ROWS = 1536
HALF = ROWS // 2
ZCH = HALF // 4
CH = ZCH // 2
KIN = 512
KOUT = 1792
K = KIN + KOUT
KH = K // 2
NB = 8
TM = 256
HA, HB, RMA, RMB, RPA, RPB, XH, D2D = range(8)
GR = 16
CR = CH + GR
UNIT = 32704.0


def nt(a, b):
    return lax.dot_general(
        a, b, (((1,), (1,)), ((), ())), precision=HIGHEST, preferred_element_type=F32
    )


def enc(x):
    codes, tops = [], []
    for i in range(CH // GR):
        part = x[i * GR : (i + 1) * GR]
        top = jnp.maximum(jnp.max(jnp.abs(part), axis=0, keepdims=True), F32(2.0**-110))
        top = jnp.ceil(jnp.log2(top))
        codes.append(jnp.round(part * (jnp.exp2(-top) * F32(UNIT))))
        tops.append(top)
    tops.append(jnp.zeros((GR - CH // GR, x.shape[1]), F32))
    rows = codes + [jnp.concatenate(tops, axis=0)]
    return jnp.concatenate(rows, axis=0).astype(jnp.int32).astype(jnp.int16)


def dec(m):
    tops = m[CH:].astype(jnp.int32).astype(F32)
    tops = jnp.exp2(tops) * F32(1.0 / UNIT)
    out = []
    for i in range(CH // GR):
        part = m[i * GR : (i + 1) * GR].astype(jnp.int32).astype(F32)
        out.append(part * tops[i : i + 1])
    return jnp.concatenate(out, axis=0)


def kernel(
    act, dl, qi, qo, ids, scores_out, docs_out,
    a_in, a_out, q, p, dbuf, sb, rb, fin, acc, cnt, oh, msga, msgb, ga, gb, dpa, dpb,
    lsem, qs, qr, rs, rr, gs, gr, ds_, dr,
):
    dp = lax.axis_index("dp")
    t = lax.axis_index("tensor")
    xl, y = dp // 4, dp % 4
    hx, z, c = t // 8, (t // 2) % 4, t % 2

    x_lo = {"dp": (dp + 4) % 8, "tensor": t}
    y_up = {"dp": xl * 4 + (y + 1) % 4, "tensor": t}
    y_dn = {"dp": xl * 4 + (y + 3) % 4, "tensor": t}
    x_hi = {"dp": dp, "tensor": (t + 8) % 16}
    z_up = {"dp": dp, "tensor": hx * 8 + ((z + 1) % 4) * 2 + c}
    z_dn = {"dp": dp, "tensor": hx * 8 + ((z + 3) % 4) * 2 + c}
    mate = {"dp": dp, "tensor": hx * 8 + z * 2 + 1 - c}

    loads = [
        pltpu.make_async_copy(qi, q.at[0, pl.ds(0, KIN)], lsem.at[0]),
        pltpu.make_async_copy(qo, q.at[0, pl.ds(KIN, KOUT)], lsem.at[1]),
        pltpu.make_async_copy(act, a_in, lsem.at[2]),
        pltpu.make_async_copy(dl, a_out, lsem.at[3]),
    ]
    for cp in loads:
        cp.start()

    barrier = pltpu.get_barrier_semaphore()
    for k in range(1, 16):
        pl.semaphore_signal(
            barrier, inc=1, device_id={"dp": dp, "tensor": (t + k) % 16}, device_id_type=MESH
        )
    for k in range(1, 8):
        pl.semaphore_signal(
            barrier, inc=1, device_id={"dp": (dp + k) % 8, "tensor": t}, device_id_type=MESH
        )

    slot = c * 8 + z * 2 + hx
    at = slot * CH
    line, off = at // 128, at % 128
    one = jnp.broadcast_to(ids[pl.ds(line, 1), :], (8, 128))
    two = jnp.broadcast_to(ids[pl.ds(jnp.minimum(line + 1, ROWS // 128 - 1), 1), :], (8, 128))
    lane = lax.broadcasted_iota(jnp.int32, (8, 128), 1)
    turn = (128 - off) % 128
    seen = jnp.where(lane < 128 - off, pltpu.roll(one, turn, 1), pltpu.roll(two, turn, 1))
    seen = jnp.where(lane < CH, seen, -1000)[:1]
    doc = lax.broadcasted_iota(jnp.int32, (128, 128), 0)
    oh[...] = (doc == seen).astype(F32)
    cnt[...] = nt(jnp.ones((8, 128), F32), (doc - 64 == seen).astype(F32))

    pl.semaphore_wait(barrier, 22)

    sent = []

    def send(src, dst, ss, rsem, to):
        cp = pltpu.make_async_remote_copy(
            src_ref=src, dst_ref=dst, send_sem=ss, recv_sem=rsem,
            device_id=to, device_id_type=MESH,
        )
        cp.start()
        sent.append(cp)
        return cp

    lo, hi, full = pl.ds(0, KH), pl.ds(KH, KH), pl.ds(0, K)

    def qsend(n, src, dst, rows, to):
        return send(q.at[src, rows], q.at[dst, rows], qs.at[n], qr.at[n], to)

    loads[0].wait()
    loads[1].wait()
    q1 = qsend(0, 0, 1, full, x_lo)
    q3 = qsend(1, 0, 3, full, y_up)
    q2 = qsend(2, 0, 2, full, y_dn)
    loads[2].wait()
    loads[3].wait()

    moves = {}

    def rsend(b, role, src, dst, to):
        moves[b, role] = send(src, dst, rs.at[role, b], rr.at[role, b], to)

    own, other = c * HALF, (1 - c) * HALF

    def code(b, role, x, to):
        sb[b, role] = enc(x)
        rsend(b, role, sb.at[b, role], rb.at[b, role], to)

    def chip(b, dz, part):
        rel = ((z + dz) % 4) * ZCH + part * CH
        rows = pl.ds(pl.multiple_of(own + rel, CH), CH)
        return p[b, rows, :] + dbuf[b, pl.ds(pl.multiple_of(rel, CH), CH), :]

    def mm(*bs):
        for base in (other, own):

            def tile(i, carry, base=base):
                rows = pl.ds(pl.multiple_of(base + i * TM, TM), TM)
                for lhs, first, deep, col in ((a_in, 0, KIN, 0), (a_out, KIN, KOUT, 128)):
                    rhs = [q[b, pl.ds(first, deep), :] for b in bs]
                    rhs = rhs[0] if len(bs) == 1 else jnp.concatenate(rhs, axis=1)
                    out = jnp.dot(lhs[rows, :], rhs, preferred_element_type=F32)
                    for i, b in enumerate(bs):
                        p[b, rows, pl.ds(col, 128)] = out[:, i * 128 : (i + 1) * 128]
                return carry

            lax.fori_loop(0, HALF // TM, tile, 0)
            if base is other:
                for b in bs:
                    rows = pl.ds(pl.multiple_of(other, HALF), HALF)
                    rsend(b, D2D, p.at[b, rows], dbuf.at[b], mate)

    def s1(b):
        moves[b, D2D].wait_recv()
        code(b, HA, chip(b, 2, 0), z_up)
        code(b, HB, chip(b, 2, 1), z_dn)
        code(b, RMB, chip(b, 1, 1), z_up)
        code(b, RPA, chip(b, 3, 0), z_dn)

    def s2(b):
        moves[b, HA].wait_recv()
        code(b, RMA, chip(b, 1, 0) + dec(rb[b, HA]), z_up)
        moves[b, HB].wait_recv()
        code(b, RPB, chip(b, 3, 1) + dec(rb[b, HB]), z_dn)

    def s3(b):
        for role in (RMB, RPA, RMA, RPB):
            moves[b, role].wait_recv()
        far = 1 - hx
        code(b, XH, chip(b, 0, far) + dec(rb[b, RMA + far]) + dec(rb[b, RPA + far]), x_hi)
        fin[b] = chip(b, 0, hx) + dec(rb[b, RMA + hx]) + dec(rb[b, RPA + hx])

    source = [
        dp, (dp + 4) % 8,
        xl * 4 + (y + 1) % 4, xl * 4 + (y + 3) % 4, xl * 4 + (y + 2) % 4,
        (1 - xl) * 4 + (y + 1) % 4, (1 - xl) * 4 + (y + 3) % 4, (1 - xl) * 4 + (y + 2) % 4,
    ]

    def s4(b):
        moves[b, XH].wait_recv()
        total = fin[b] + dec(rb[b, XH])
        prod = total[:, :128] * total[:, 128:]
        prod = jnp.concatenate([prod, jnp.zeros((128 - CH, 128), F32)], axis=0)
        row = lax.broadcasted_iota(jnp.int32, (8, 128), 0)
        col = lax.broadcasted_iota(jnp.int32, (8, 128), 1)
        pick = jnp.where(row == (b % 2) * 4 + col // RANK, F32(RANK ** -0.5), F32(0))
        acc[b] = nt(pick, prod)

    def share(first, last, msg, g, n):
        rows = (last - first) * 4
        for b in range(first, last, 2):
            msg[pl.ds((b - first) * 4, 8), :] = acc[b] + acc[b + 1]
        mine = msg[pl.ds(0, rows), :]
        msg[pl.ds(rows, rows), :] = nt(mine, oh[...]) + jnp.broadcast_to(cnt[:1], (rows, 128))
        g[slot] = msg[...]
        got = []
        for k in range(1, 16):
            to = {"dp": dp, "tensor": (t + k) % 16}
            got.append(send(msg, g.at[slot], gs.at[n, k - 1], gr.at[n, k - 1], to))
        return got

    def rows_of(first, last, found, out, source=source):
        row = lax.broadcasted_iota(jnp.int32, out.shape, 0)
        for b in range(first, last):
            for j in range(4):
                i = (b - first) * 4 + j
                line = jnp.broadcast_to(found[i : i + 1], out.shape)
                out = jnp.where(row == source[b] * 4 + j, line, out)
        return out

    def total(got, g, buf, n, spread):
        for cp in got:
            cp.wait_recv()
        rows = g.shape[1] // 2
        part = g[0, pl.ds(rows, rows), :]
        for m in range(1, 16):
            part = part + g[m, pl.ds(rows, rows), :]
        buf[dp] = spread(part)
        got = []
        for k in range(1, 8):
            to = {"dp": (dp + k) % 8, "tensor": t}
            got.append(send(buf.at[dp], buf.at[dp], ds_.at[n, k - 1], dr.at[n, k - 1], to))
        return got

    def place(first, last, g):
        rows = (last - first) * 4
        found = jnp.concatenate([g[m, pl.ds(0, rows), :][:, :CH] for m in range(16)], axis=1)
        old = jnp.zeros((32, ROWS), F32) if first == 0 else scores_out[...]
        scores_out[...] = rows_of(first, last, found, old)

    def mean(early, late):
        for cp in early:
            cp.wait_recv()
        whole = dpa[0]
        for m in range(1, 8):
            whole = whole + dpa[m]
        for cp in late:
            cp.wait_recv()
        for m in range(8):
            where = [(1 - m // 4) * 4 + (m + 3) % 4, (1 - m // 4) * 4 + (m + 2) % 4]
            whole = whole + rows_of(0, 2, dpb[m], jnp.zeros((32, 128), F32), where)
        docs_out[...] = (whole / pltpu.roll(whole, 64, 1))[:, :64]

    mm(0)
    s1(0)
    s2(0)
    s3(0)

    q3.wait_recv()
    q4a = qsend(3, 3, 4, lo, y_up)
    q2.wait_recv()
    q4b = qsend(4, 2, 4, hi, y_dn)
    q5a = qsend(5, 2, 5, lo, x_lo)
    q5b = qsend(6, 2, 5, hi, x_lo)
    q1.wait_recv()
    q6 = qsend(7, 1, 6, full, y_up)
    mm(1, 2)
    s1(1)
    s1(2)
    mm(3)
    q5a.wait_recv()
    q7a = qsend(8, 5, 7, lo, y_dn)
    s2(1)
    s1(3)
    s2(2)
    s4(0)
    q4a.wait_recv()
    q4b.wait_recv()
    mm(4)
    s3(1)
    s2(3)
    s1(4)
    s3(2)
    q5b.wait_recv()
    q7b = qsend(9, 5, 7, hi, y_dn)
    mm(5)
    s4(1)
    s3(3)
    s2(4)
    s1(5)
    s4(2)
    s3(4)
    s2(5)
    s4(3)
    s4(4)
    s3(5)
    q6.wait_recv()
    q7a.wait_recv()
    q7b.wait_recv()
    mm(6, 7)
    s4(5)
    share_a = share(0, 6, msga, ga, 0)
    s1(6)
    s1(7)
    s2(6)
    s2(7)
    total_a = total(share_a, ga, dpa, 0, lambda v: rows_of(0, 6, v, jnp.zeros((32, 128), F32)))
    s3(6)
    s3(7)
    place(0, 6, ga)
    s4(6)
    s4(7)
    share_b = share(6, 8, msgb, gb, 1)
    total_b = total(share_b, gb, dpb, 1, lambda v: v)
    place(6, 8, gb)
    mean(total_a, total_b)
    for cp in sent:
        cp.wait_send()


def body(activations, deltas, query_in, query_out, doc_ids):
    ids = doc_ids.reshape(ROWS // 128, 128)
    any_ = pl.BlockSpec(memory_space=pl.ANY)
    vmem = pl.BlockSpec(memory_space=pltpu.VMEM)
    dma = pltpu.SemaphoreType.DMA
    scores, docs = pl.pallas_call(
        kernel,
        out_shape=(
            jax.ShapeDtypeStruct((32, ROWS), F32),
            jax.ShapeDtypeStruct((32, 64), F32),
        ),
        in_specs=[any_, any_, any_, any_, vmem],
        out_specs=(vmem, vmem),
        scratch_shapes=[
            pltpu.VMEM((ROWS, KIN), jnp.bfloat16),
            pltpu.VMEM((ROWS, KOUT), jnp.bfloat16),
            pltpu.VMEM((NB, K, 128), jnp.bfloat16),
            pltpu.VMEM((NB, ROWS, 256), F32),
            pltpu.VMEM((NB, HALF, 256), F32),
            pltpu.VMEM((NB, 7, CR, 256), jnp.int16),
            pltpu.VMEM((NB, 7, CR, 256), jnp.int16),
            pltpu.VMEM((NB, CH, 256), F32),
            pltpu.VMEM((NB, 8, 128), F32),
            pltpu.VMEM((8, 128), F32),
            pltpu.VMEM((128, 128), F32),
            pltpu.VMEM((48, 128), F32),
            pltpu.VMEM((16, 128), F32),
            pltpu.VMEM((16, 48, 128), F32),
            pltpu.VMEM((16, 16, 128), F32),
            pltpu.VMEM((8, 32, 128), F32),
            pltpu.VMEM((8, 8, 128), F32),
            dma((4,)), dma((10,)), dma((10,)), dma((8, NB)), dma((8, NB)),
            dma((2, 15)), dma((2, 15)), dma((2, 7)), dma((2, 7)),
        ],
        compiler_params=pltpu.CompilerParams(
            collective_id=0, has_side_effects=True, vmem_limit_bytes=60 * 1024 * 1024
        ),
    )(activations, deltas, query_in, query_out, ids)
    return scores.T, docs.T


def solution(mesh):
    return jax.shard_map(
        body,
        mesh=mesh,
        in_specs=(
            P("dp", "tensor"),
            P("dp", "tensor"),
            P("tensor", "dp"),
            P("tensor", "dp"),
            P("dp"),
        ),
        out_specs=(P("dp", None), P()),
        check_vma=False,
    )
```

```python
import jax
import jax.numpy as jnp
from jax import lax
from jax.experimental import pallas as pl
from jax.experimental.pallas import tpu as pltpu
from jax.sharding import PartitionSpec as P

RANK = 32
MESH = pl.DeviceIdType.MESH
F32 = jnp.float32
HIGHEST = lax.Precision.HIGHEST

ROWS = 1536
HALF = ROWS // 2
ZCH = HALF // 4
CH = ZCH // 2
KIN = 512
KOUT = 1792
K = KIN + KOUT
KH = K // 2
NB = 8
TM = 256
HA, HB, RMA, RMB, RPA, RPB, XH = range(7)
KQ = K // 4
GR = 16
CR = CH + GR
UNIT = 32704.0


def nt(a, b):
    return lax.dot_general(
        a, b, (((1,), (1,)), ((), ())), precision=HIGHEST, preferred_element_type=F32
    )


def enc(x):
    codes, tops = [], []
    for i in range(CH // GR):
        part = x[i * GR : (i + 1) * GR]
        top = jnp.maximum(jnp.max(jnp.abs(part), axis=0, keepdims=True), F32(2.0**-110))
        top = jnp.ceil(jnp.log2(top))
        codes.append(jnp.round(part * (jnp.exp2(-top) * F32(UNIT))))
        tops.append(top)
    tops.append(jnp.zeros((GR - CH // GR, x.shape[1]), F32))
    rows = codes + [jnp.concatenate(tops, axis=0)]
    return jnp.concatenate(rows, axis=0).astype(jnp.int32).astype(jnp.int16)


def dec(m):
    tops = m[CH:].astype(jnp.int32).astype(F32)
    tops = jnp.exp2(tops) * F32(1.0 / UNIT)
    out = []
    for i in range(CH // GR):
        part = m[i * GR : (i + 1) * GR].astype(jnp.int32).astype(F32)
        out.append(part * tops[i : i + 1])
    return jnp.concatenate(out, axis=0)


def kernel(
    act, dl, qi, qo, ids, scores_out, docs_out,
    a_in, a_out, q, p, dbuf, sb, rb, fin, acc, cnt, oh, every, msga, msgb, ga, gb, dpa, dpb,
    lsem, qs, qr, rs, rr, ms, mr, gs, gr, ds_, dr,
):
    dp = lax.axis_index("dp")
    t = lax.axis_index("tensor")
    xl, y = dp // 4, dp % 4
    hx, z, c = t // 8, (t // 2) % 4, t % 2

    x_lo = {"dp": (dp + 4) % 8, "tensor": t}
    y_up = {"dp": xl * 4 + (y + 1) % 4, "tensor": t}
    y_dn = {"dp": xl * 4 + (y + 3) % 4, "tensor": t}
    x_hi = {"dp": dp, "tensor": (t + 8) % 16}
    z_up = {"dp": dp, "tensor": hx * 8 + ((z + 1) % 4) * 2 + c}
    z_dn = {"dp": dp, "tensor": hx * 8 + ((z + 3) % 4) * 2 + c}
    mate = {"dp": dp, "tensor": hx * 8 + z * 2 + 1 - c}

    loads = [
        pltpu.make_async_copy(qi, q.at[0, pl.ds(0, KIN)], lsem.at[0]),
        pltpu.make_async_copy(qo, q.at[0, pl.ds(KIN, KOUT)], lsem.at[1]),
        pltpu.make_async_copy(act, a_in, lsem.at[2]),
        pltpu.make_async_copy(dl, a_out, lsem.at[3]),
    ]
    for cp in loads:
        cp.start()

    barrier = pltpu.get_barrier_semaphore()
    for k in range(1, 16):
        pl.semaphore_signal(
            barrier, inc=1, device_id={"dp": dp, "tensor": (t + k) % 16}, device_id_type=MESH
        )
    for k in range(1, 8):
        pl.semaphore_signal(
            barrier, inc=1, device_id={"dp": (dp + k) % 8, "tensor": t}, device_id_type=MESH
        )

    slot = c * 8 + z * 2 + hx
    at = slot * CH
    line, off = at // 128, at % 128
    one = jnp.broadcast_to(ids[pl.ds(line, 1), :], (8, 128))
    two = jnp.broadcast_to(ids[pl.ds(jnp.minimum(line + 1, ROWS // 128 - 1), 1), :], (8, 128))
    lane = lax.broadcasted_iota(jnp.int32, (8, 128), 1)
    turn = (128 - off) % 128
    seen = jnp.where(lane < 128 - off, pltpu.roll(one, turn, 1), pltpu.roll(two, turn, 1))
    seen = jnp.where(lane < CH, seen, -1000)[:1]
    doc = lax.broadcasted_iota(jnp.int32, (128, 128), 0)
    oh[...] = (doc == seen).astype(F32)
    cnt[...] = nt(jnp.ones((8, 128), F32), (doc - 64 == seen).astype(F32))
    for i in range(ROWS // 128):
        group = ids[pl.ds(i, 1), :]
        every[:, pl.ds(i * 128, 128)] = (doc == group).astype(jnp.bfloat16)

    pl.semaphore_wait(barrier, 22)

    sent = []

    def send(src, dst, ss, rsem, to):
        cp = pltpu.make_async_remote_copy(
            src_ref=src, dst_ref=dst, send_sem=ss, recv_sem=rsem,
            device_id=to, device_id_type=MESH,
        )
        cp.start()
        sent.append(cp)
        return cp

    lo, hi = pl.ds(0, KH), pl.ds(KH, KH)
    quarter = [pl.ds(i * KQ, KQ) for i in (2, 3, 0, 1)]

    def qsend(n, src, dst, rows, to):
        return send(q.at[src, rows], q.at[dst, rows], qs.at[n], qr.at[n], to)

    loads[0].wait()
    loads[1].wait()
    q1a = qsend(0, 0, 1, lo, x_lo)
    q3a = qsend(1, 0, 3, lo, y_up)
    q2b = qsend(2, 0, 2, hi, y_dn)
    q1b = qsend(3, 0, 1, hi, x_lo)
    q3b = qsend(4, 0, 3, hi, y_up)
    q2a = qsend(5, 0, 2, lo, y_dn)
    loads[2].wait()
    loads[3].wait()

    moves = {}

    def rsend(b, role, src, dst, to):
        moves[b, role] = send(src, dst, rs.at[role, b], rr.at[role, b], to)

    own, other = c * HALF, (1 - c) * HALF

    def code(b, role, x, to):
        sb[b, role] = enc(x)
        rsend(b, role, sb.at[b, role], rb.at[b, role], to)

    def chip(b, dz, part):
        rel = ((z + dz) % 4) * ZCH + part * CH
        rows = pl.ds(pl.multiple_of(own + rel, CH), CH)
        return p[b, rows, :] + dbuf[b, pl.ds(pl.multiple_of(rel, CH), CH), :]

    def tile(bs, rows):
        for lhs, first, deep, col in ((a_in, 0, KIN, 0), (a_out, KIN, KOUT, 128)):
            rhs = [q[b, pl.ds(first, deep), :] for b in bs]
            rhs = rhs[0] if len(bs) == 1 else jnp.concatenate(rhs, axis=1)
            out = jnp.dot(lhs[rows, :], rhs, preferred_element_type=F32)
            for i, b in enumerate(bs):
                p[b, rows, pl.ds(col, 128)] = out[:, i * 128 : (i + 1) * 128]

    pieces = HALF // TM

    def piece(b, i, start=False):
        rows = pl.ds(pl.multiple_of(other + i * TM, TM), TM)
        cp = pltpu.make_async_remote_copy(
            src_ref=p.at[b, rows],
            dst_ref=dbuf.at[b, pl.ds(pl.multiple_of(i * TM, TM), TM)],
            send_sem=ms.at[b, i], recv_sem=mr.at[b, i],
            device_id=mate, device_id_type=MESH,
        )
        if start:
            cp.start()
        return cp

    def mm(*bs):
        def first(i, carry):
            tile(bs, pl.ds(pl.multiple_of(other + i * TM, TM), TM))
            for b in bs:
                piece(b, i, True)
            return carry

        def rest(i, carry):
            tile(bs, pl.ds(pl.multiple_of(own + i * TM, TM), TM))
            return carry

        lax.fori_loop(0, pieces, first, 0)
        lax.fori_loop(0, pieces, rest, 0)
        for b in bs:
            for i in range(pieces):
                moves[b, "core", i] = piece(b, i)
                sent.append(moves[b, "core", i])

    def s1(b):
        for i in range(pieces):
            moves[b, "core", i].wait_recv()
        code(b, HA, chip(b, 2, 0), z_up)
        code(b, HB, chip(b, 2, 1), z_dn)
        code(b, RMB, chip(b, 1, 1), z_up)
        code(b, RPA, chip(b, 3, 0), z_dn)

    def s2(b):
        moves[b, HA].wait_recv()
        code(b, RMA, chip(b, 1, 0) + dec(rb[b, HA]), z_up)
        moves[b, HB].wait_recv()
        code(b, RPB, chip(b, 3, 1) + dec(rb[b, HB]), z_dn)

    def s3(b):
        for role in (RMB, RPA, RMA, RPB):
            moves[b, role].wait_recv()
        far = 1 - hx
        code(b, XH, chip(b, 0, far) + dec(rb[b, RMA + far]) + dec(rb[b, RPA + far]), x_hi)
        fin[b] = chip(b, 0, hx) + dec(rb[b, RMA + hx]) + dec(rb[b, RPA + hx])

    source = [
        dp, (dp + 4) % 8,
        xl * 4 + (y + 1) % 4, xl * 4 + (y + 3) % 4, xl * 4 + (y + 2) % 4,
        (1 - xl) * 4 + (y + 1) % 4, (1 - xl) * 4 + (y + 3) % 4, (1 - xl) * 4 + (y + 2) % 4,
    ]

    def s4(b):
        moves[b, XH].wait_recv()
        total = fin[b] + dec(rb[b, XH])
        prod = total[:, :128] * total[:, 128:]
        prod = jnp.concatenate([prod, jnp.zeros((128 - CH, 128), F32)], axis=0)
        row = lax.broadcasted_iota(jnp.int32, (8, 128), 0)
        col = lax.broadcasted_iota(jnp.int32, (8, 128), 1)
        pick = jnp.where(row == (b % 2) * 4 + col // RANK, F32(RANK ** -0.5), F32(0))
        acc[b] = nt(pick, prod)

    def spread(msg, g, n):
        g[slot] = msg[...]
        got = []
        for k in range(1, 16):
            to = {"dp": dp, "tensor": (t + k) % 16}
            got.append(send(msg, g.at[slot], gs.at[n, k - 1], gr.at[n, k - 1], to))
        return got

    def share_a():
        for b in range(0, 6, 2):
            msga[pl.ds(b * 4, 8), :] = acc[b] + acc[b + 1]
        return spread(msga, ga, 0)

    def share_b():
        mine = acc[6] + acc[7]
        msgb[pl.ds(0, 8), :] = mine
        msgb[pl.ds(8, 8), :] = nt(mine, oh[...]) + cnt[...]
        return spread(msgb, gb, 1)

    def rows_of(first, last, found, out, source=source):
        row = lax.broadcasted_iota(jnp.int32, out.shape, 0)
        for b in range(first, last):
            for j in range(4):
                i = (b - first) * 4 + j
                line = jnp.broadcast_to(found[i : i + 1], out.shape)
                out = jnp.where(row == source[b] * 4 + j, line, out)
        return out

    def gathered(g, rows):
        return jnp.concatenate([g[m, pl.ds(0, rows), :][:, :CH] for m in range(16)], axis=1)

    def finish_a(got):
        for cp in got:
            cp.wait_recv()
        found = gathered(ga, 24)
        scores_out[...] = rows_of(0, 6, found, jnp.zeros((32, ROWS), F32))
        one = found.astype(jnp.bfloat16)
        left = found - one.astype(F32)
        two = left.astype(jnp.bfloat16)
        three = (left - two.astype(F32)).astype(jnp.bfloat16)
        sums = jnp.zeros((24, 128), F32)
        for part in (three, two, one):
            sums = sums + lax.dot_general(
                part, every[...], (((1,), (1,)), ((), ())), preferred_element_type=F32
            )
        return across(dpa, rows_of(0, 6, sums, jnp.zeros((32, 128), F32)), 0)

    def finish_b(got):
        for cp in got:
            cp.wait_recv()
        part = gb[0, pl.ds(8, 8), :]
        for m in range(1, 16):
            part = part + gb[m, pl.ds(8, 8), :]
        return across(dpb, part, 1)

    def across(buf, part, n):
        buf[dp] = part
        got = []
        for k in range(1, 8):
            to = {"dp": (dp + k) % 8, "tensor": t}
            got.append(send(buf.at[dp], buf.at[dp], ds_.at[n, k - 1], dr.at[n, k - 1], to))
        return got

    def mean(early, late):
        for cp in early:
            cp.wait_recv()
        whole = dpa[0]
        for m in range(1, 8):
            whole = whole + dpa[m]
        for cp in late:
            cp.wait_recv()
        for m in range(8):
            where = [(1 - m // 4) * 4 + (m + 3) % 4, (1 - m // 4) * 4 + (m + 2) % 4]
            whole = whole + rows_of(0, 2, dpb[m], jnp.zeros((32, 128), F32), where)
        held = dpb[0, pl.ds(0, 1), :]
        for m in range(1, 8):
            held = held + dpb[m, pl.ds(0, 1), :]
        held = jnp.broadcast_to(pltpu.roll(jnp.broadcast_to(held, (8, 128)), 64, 1)[:1], (32, 128))
        docs_out[...] = (whole / held)[:, :64]

    def forward(n):
        q5[n].wait_recv()
        q7.append(qsend(14 + n, 5, 7, quarter[n], y_dn))

    mm(0)
    s1(0)
    s2(0)
    q3a.wait_recv()
    q4a = qsend(6, 3, 4, lo, y_up)
    q2b.wait_recv()
    q4b = qsend(7, 2, 4, hi, y_dn)
    q5 = [qsend(10, 2, 5, quarter[0], x_lo), qsend(11, 2, 5, quarter[1], x_lo)]
    q7 = []
    q1a.wait_recv()
    q6a = qsend(8, 1, 6, lo, y_up)
    s3(0)
    q2a.wait_recv()
    q5 += [qsend(12, 2, 5, quarter[2], x_lo), qsend(13, 2, 5, quarter[3], x_lo)]
    q1b.wait_recv()
    q6b = qsend(9, 1, 6, hi, y_up)
    mm(1, 2)
    forward(0)
    s1(1)
    s1(2)
    q3b.wait_recv()
    mm(3)
    forward(1)
    s2(1)
    s1(3)
    forward(2)
    q4a.wait_recv()
    q4b.wait_recv()
    mm(4)
    s2(2)
    forward(3)
    s1(4)
    s3(1)
    s2(3)
    mm(5)
    s3(2)
    s1(5)
    s4(0)
    s2(4)
    s3(3)
    for cp in (q6a, q6b, *q7):
        cp.wait_recv()
    mm(6, 7)
    s4(1)
    s4(2)
    s2(5)
    s3(4)
    s1(6)
    s1(7)
    s4(3)
    s3(5)
    s2(6)
    s4(4)
    s2(7)
    s4(5)
    s3(6)
    s3(7)
    shared_a = share_a()
    s4(6)
    s4(7)
    shared_b = share_b()
    early = finish_a(shared_a)
    late = finish_b(shared_b)
    scores_out[...] = rows_of(6, 8, gathered(gb, 8), scores_out[...])
    mean(early, late)
    for cp in sent:
        cp.wait_send()


def body(activations, deltas, query_in, query_out, doc_ids):
    ids = doc_ids.reshape(ROWS // 128, 128)
    any_ = pl.BlockSpec(memory_space=pl.ANY)
    vmem = pl.BlockSpec(memory_space=pltpu.VMEM)
    dma = pltpu.SemaphoreType.DMA
    scores, docs = pl.pallas_call(
        kernel,
        out_shape=(
            jax.ShapeDtypeStruct((32, ROWS), F32),
            jax.ShapeDtypeStruct((32, 64), F32),
        ),
        in_specs=[any_, any_, any_, any_, vmem],
        out_specs=(vmem, vmem),
        scratch_shapes=[
            pltpu.VMEM((ROWS, KIN), jnp.bfloat16),
            pltpu.VMEM((ROWS, KOUT), jnp.bfloat16),
            pltpu.VMEM((NB, K, 128), jnp.bfloat16),
            pltpu.VMEM((NB, ROWS, 256), F32),
            pltpu.VMEM((NB, HALF, 256), F32),
            pltpu.VMEM((NB, 7, CR, 256), jnp.int16),
            pltpu.VMEM((NB, 7, CR, 256), jnp.int16),
            pltpu.VMEM((NB, CH, 256), F32),
            pltpu.VMEM((NB, 8, 128), F32),
            pltpu.VMEM((8, 128), F32),
            pltpu.VMEM((128, 128), F32),
            pltpu.VMEM((128, ROWS), jnp.bfloat16),
            pltpu.VMEM((24, 128), F32),
            pltpu.VMEM((16, 128), F32),
            pltpu.VMEM((16, 24, 128), F32),
            pltpu.VMEM((16, 16, 128), F32),
            pltpu.VMEM((8, 32, 128), F32),
            pltpu.VMEM((8, 8, 128), F32),
            dma((4,)), dma((18,)), dma((18,)), dma((7, NB)), dma((7, NB)),
            dma((NB, HALF // TM)), dma((NB, HALF // TM)),
            dma((2, 15)), dma((2, 15)), dma((2, 7)), dma((2, 7)),
        ],
        compiler_params=pltpu.CompilerParams(
            collective_id=0, has_side_effects=True, vmem_limit_bytes=60 * 1024 * 1024
        ),
    )(activations, deltas, query_in, query_out, ids)
    def finish(a, b, oa, ob):
        oa[...] = a[...]
        ob[...] = b[...]

    scores, docs = pl.pallas_call(
        finish,
        out_shape=(
            jax.ShapeDtypeStruct((32, ROWS), F32),
            jax.ShapeDtypeStruct((32, 64), F32),
        ),
        in_specs=[vmem, vmem],
        out_specs=(vmem, vmem),
    )(scores, docs)
    return scores.T, docs.T


def solution(mesh):
    return jax.shard_map(
        body,
        mesh=mesh,
        in_specs=(
            P("dp", "tensor"),
            P("dp", "tensor"),
            P("tensor", "dp"),
            P("tensor", "dp"),
            P("dp"),
        ),
        out_specs=(P("dp", None), P()),
        check_vma=False,
    )
```

```python
import jax
import jax.numpy as jnp
from jax import lax
from jax.experimental import pallas as pl
from jax.experimental.pallas import tpu as pltpu
from jax.sharding import PartitionSpec as P

RANK = 32
MESH = pl.DeviceIdType.MESH
F32 = jnp.float32
HIGHEST = lax.Precision.HIGHEST

ROWS = 1536
HALF = ROWS // 2
ZCH = HALF // 4
CH = ZCH // 2
KIN = 512
KOUT = 1792
K = KIN + KOUT
KH = K // 2
NB = 8
TM = 256
HA, HB, RMA, RMB, RPA, RPB, XH = range(7)
KQ = K // 4
GR = 16
CR = CH + 8
UNIT = 32704.0


def nt(a, b):
    return lax.dot_general(
        a, b, (((1,), (1,)), ((), ())), precision=HIGHEST, preferred_element_type=F32
    )


def enc(x):
    codes, tops = [], []
    for i in range(CH // GR):
        part = x[i * GR : (i + 1) * GR]
        top = jnp.maximum(jnp.max(jnp.abs(part), axis=0, keepdims=True), F32(2.0**-110))
        top = jnp.ceil(jnp.log2(top))
        codes.append(jnp.round(part * (jnp.exp2(-top) * F32(UNIT))))
        tops.append(top)
    tops.append(jnp.zeros((8 - CH // GR, x.shape[1]), F32))
    rows = codes + [jnp.concatenate(tops, axis=0)]
    return jnp.concatenate(rows, axis=0).astype(jnp.int32).astype(jnp.int16)


def dec(m):
    tops = m[CH:].astype(jnp.int32).astype(F32)
    tops = jnp.exp2(tops) * F32(1.0 / UNIT)
    out = []
    for i in range(CH // GR):
        part = m[i * GR : (i + 1) * GR].astype(jnp.int32).astype(F32)
        out.append(part * tops[i : i + 1])
    return jnp.concatenate(out, axis=0)


def kernel(
    act, dl, qi, qo, ids_in, scores_out, docs_out,
    a_in, a_out, q, p, dbuf, sb, rb, fin, acc, cnt, oh, every, ids, msga, msgb, ga, gb, dpa, dpb,
    lsem, qs, qr, rs, rr, ms, mr, gs, gr, ds_, dr,
):
    dp = lax.axis_index("dp")
    t = lax.axis_index("tensor")
    xl, y = dp // 4, dp % 4
    hx, z, c = t // 8, (t // 2) % 4, t % 2

    x_lo = {"dp": (dp + 4) % 8, "tensor": t}
    y_up = {"dp": xl * 4 + (y + 1) % 4, "tensor": t}
    y_dn = {"dp": xl * 4 + (y + 3) % 4, "tensor": t}
    x_hi = {"dp": dp, "tensor": (t + 8) % 16}
    z_up = {"dp": dp, "tensor": hx * 8 + ((z + 1) % 4) * 2 + c}
    z_dn = {"dp": dp, "tensor": hx * 8 + ((z + 3) % 4) * 2 + c}
    mate = {"dp": dp, "tensor": hx * 8 + z * 2 + 1 - c}

    loads = [
        pltpu.make_async_copy(qi, q.at[0, pl.ds(0, KIN)], lsem.at[0]),
        pltpu.make_async_copy(qo, q.at[0, pl.ds(KIN, KOUT)], lsem.at[1]),
        pltpu.make_async_copy(act, a_in, lsem.at[2]),
        pltpu.make_async_copy(dl, a_out, lsem.at[3]),
        pltpu.make_async_copy(ids_in, ids, lsem.at[4]),
    ]
    for cp in loads:
        cp.start()

    barrier = pltpu.get_barrier_semaphore()
    near = (x_lo, y_up, y_dn, x_hi, z_up, z_dn, mate)
    for to in near:
        pl.semaphore_signal(barrier, inc=1, device_id=to, device_id_type=MESH)
    pl.semaphore_wait(barrier, len(near))

    sent = []

    def send(src, dst, ss, rsem, to):
        cp = pltpu.make_async_remote_copy(
            src_ref=src, dst_ref=dst, send_sem=ss, recv_sem=rsem,
            device_id=to, device_id_type=MESH,
        )
        cp.start()
        sent.append(cp)
        return cp

    lo, hi = pl.ds(0, KH), pl.ds(KH, KH)
    quarter = [pl.ds(i * KQ, KQ) for i in (2, 3, 0, 1)]

    def qsend(n, src, dst, rows, to):
        return send(q.at[src, rows], q.at[dst, rows], qs.at[n], qr.at[n], to)

    loads[0].wait()
    loads[1].wait()
    q1a = qsend(0, 0, 1, lo, x_lo)
    q3a = qsend(1, 0, 3, lo, y_up)
    q2b = qsend(2, 0, 2, hi, y_dn)
    q1b = qsend(3, 0, 1, hi, x_lo)
    q3b = qsend(4, 0, 3, hi, y_up)
    q2a = qsend(5, 0, 2, lo, y_dn)

    slot = c * 8 + z * 2 + hx

    moves = {}

    def rsend(b, role, src, dst, to):
        moves[b, role] = send(src, dst, rs.at[role, b], rr.at[role, b], to)

    own, other = c * HALF, (1 - c) * HALF

    def code(b, role, x, to):
        sb[b, role] = enc(x)
        rsend(b, role, sb.at[b, role], rb.at[b, role], to)

    def chip(b, dz, part):
        rel = ((z + dz) % 4) * ZCH + part * CH
        rows = pl.ds(pl.multiple_of(own + rel, CH), CH)
        return p[b, rows, :] + dbuf[b, pl.ds(pl.multiple_of(rel, CH), CH), :]

    def tile(bs, rows):
        for lhs, first, deep, col in ((a_in, 0, KIN, 0), (a_out, KIN, KOUT, 128)):
            rhs = [q[b, pl.ds(first, deep), :] for b in bs]
            rhs = rhs[0] if len(bs) == 1 else jnp.concatenate(rhs, axis=1)
            out = jnp.dot(lhs[rows, :], rhs, preferred_element_type=F32)
            for i, b in enumerate(bs):
                p[b, rows, pl.ds(col, 128)] = out[:, i * 128 : (i + 1) * 128]

    pieces = HALF // TM

    def piece(b, i, start=False):
        rows = pl.ds(pl.multiple_of(other + i * TM, TM), TM)
        cp = pltpu.make_async_remote_copy(
            src_ref=p.at[b, rows],
            dst_ref=dbuf.at[b, pl.ds(pl.multiple_of(i * TM, TM), TM)],
            send_sem=ms.at[b, i], recv_sem=mr.at[b, i],
            device_id=mate, device_id_type=MESH,
        )
        if start:
            cp.start()
        return cp

    def mm(*bs, between=lambda: None):
        def first(i, carry):
            tile(bs, pl.ds(pl.multiple_of(other + i * TM, TM), TM))
            for b in bs:
                piece(b, i, True)
            return carry

        def rest(i, carry):
            tile(bs, pl.ds(pl.multiple_of(own + i * TM, TM), TM))
            return carry

        lax.fori_loop(0, pieces, first, 0)
        between()
        lax.fori_loop(0, pieces, rest, 0)
        for b in bs:
            for i in range(pieces):
                moves[b, "core", i] = piece(b, i)
                sent.append(moves[b, "core", i])

    def s1(b):
        for i in range(pieces):
            moves[b, "core", i].wait_recv()
        code(b, HA, chip(b, 2, 0), z_up)
        code(b, HB, chip(b, 2, 1), z_dn)

    def s1b(b):
        code(b, RMB, chip(b, 1, 1), z_up)
        code(b, RPA, chip(b, 3, 0), z_dn)

    def s2(b):
        moves[b, HA].wait_recv()
        code(b, RMA, chip(b, 1, 0) + dec(rb[b, HA]), z_up)
        moves[b, HB].wait_recv()
        code(b, RPB, chip(b, 3, 1) + dec(rb[b, HB]), z_dn)

    def s3(b):
        for role in (RMB, RPA, RMA, RPB):
            moves[b, role].wait_recv()
        far = 1 - hx
        code(b, XH, chip(b, 0, far) + dec(rb[b, RMA + far]) + dec(rb[b, RPA + far]), x_hi)
        fin[b] = chip(b, 0, hx) + dec(rb[b, RMA + hx]) + dec(rb[b, RPA + hx])

    source = [
        dp, (dp + 4) % 8,
        xl * 4 + (y + 1) % 4, xl * 4 + (y + 3) % 4, xl * 4 + (y + 2) % 4,
        (1 - xl) * 4 + (y + 1) % 4, (1 - xl) * 4 + (y + 3) % 4, (1 - xl) * 4 + (y + 2) % 4,
    ]

    def s4(b):
        moves[b, XH].wait_recv()
        total = fin[b] + dec(rb[b, XH])
        prod = total[:, :128] * total[:, 128:]
        prod = jnp.concatenate([prod, jnp.zeros((128 - CH, 128), F32)], axis=0)
        row = lax.broadcasted_iota(jnp.int32, (8, 128), 0)
        col = lax.broadcasted_iota(jnp.int32, (8, 128), 1)
        pick = jnp.where(row == (b % 2) * 4 + col // RANK, F32(RANK ** -0.5), F32(0))
        acc[b] = nt(pick, prod)

    def spread(msg, g, n):
        g[slot] = msg[...]
        got = []
        for k in range(1, 16):
            to = {"dp": dp, "tensor": (t + k) % 16}
            got.append(send(msg, g.at[slot], gs.at[n, k - 1], gr.at[n, k - 1], to))
        return got

    def share_a():
        for b in range(0, 6, 2):
            msga[pl.ds(b * 4, 8), :] = acc[b] + acc[b + 1]
        return spread(msga, ga, 0)

    def share_b():
        mine = acc[6] + acc[7]
        msgb[pl.ds(0, 8), :] = mine
        msgb[pl.ds(8, 8), :] = nt(mine, oh[...]) + cnt[...]
        return spread(msgb, gb, 1)

    def rows_of(first, last, found, out, source=source):
        row = lax.broadcasted_iota(jnp.int32, out.shape, 0)
        for b in range(first, last):
            for j in range(4):
                i = (b - first) * 4 + j
                line = jnp.broadcast_to(found[i : i + 1], out.shape)
                out = jnp.where(row == source[b] * 4 + j, line, out)
        return out

    def gathered(g, rows):
        return jnp.concatenate([g[m, pl.ds(0, rows), :][:, :CH] for m in range(16)], axis=1)

    def finish_a(got):
        for cp in got:
            cp.wait_recv()
        found = gathered(ga, 24)
        scores_out[...] = rows_of(0, 6, found, jnp.zeros((32, ROWS), F32))
        one = found.astype(jnp.bfloat16)
        left = found - one.astype(F32)
        two = left.astype(jnp.bfloat16)
        three = (left - two.astype(F32)).astype(jnp.bfloat16)
        sums = jnp.zeros((24, 128), F32)
        for part in (three, two, one):
            sums = sums + lax.dot_general(
                part, every[...], (((1,), (1,)), ((), ())), preferred_element_type=F32
            )
        return across(dpa, rows_of(0, 6, sums, jnp.zeros((32, 128), F32)), 0)

    def finish_b(got):
        for cp in got:
            cp.wait_recv()
        part = gb[0, pl.ds(8, 8), :]
        for m in range(1, 16):
            part = part + gb[m, pl.ds(8, 8), :]
        return across(dpb, part, 1)

    def across(buf, part, n):
        buf[dp] = part
        got = []
        for k in range(1, 8):
            to = {"dp": (dp + k) % 8, "tensor": t}
            got.append(send(buf.at[dp], buf.at[dp], ds_.at[n, k - 1], dr.at[n, k - 1], to))
        return got

    def mean(early, late):
        for cp in early:
            cp.wait_recv()
        whole = dpa[0]
        for m in range(1, 8):
            whole = whole + dpa[m]
        for cp in late:
            cp.wait_recv()
        for m in range(8):
            where = [(1 - m // 4) * 4 + (m + 3) % 4, (1 - m // 4) * 4 + (m + 2) % 4]
            whole = whole + rows_of(0, 2, dpb[m], jnp.zeros((32, 128), F32), where)
        held = dpb[0, pl.ds(0, 1), :]
        for m in range(1, 8):
            held = held + dpb[m, pl.ds(0, 1), :]
        held = jnp.broadcast_to(pltpu.roll(jnp.broadcast_to(held, (8, 128)), 64, 1)[:1], (32, 128))
        docs_out[...] = (whole / held)[:, :64]

    def forward(n):
        q5[n].wait_recv()
        q7.append(qsend(14 + n, 5, 7, quarter[n], y_dn))

    loads[2].wait()
    loads[3].wait()
    mm(0)
    s1(0)
    s1b(0)
    loads[4].wait()
    at = slot * CH
    line, off = at // 128, at % 128
    one = jnp.broadcast_to(ids[pl.ds(line, 1), :], (8, 128))
    two = jnp.broadcast_to(ids[pl.ds(jnp.minimum(line + 1, ROWS // 128 - 1), 1), :], (8, 128))
    lane = lax.broadcasted_iota(jnp.int32, (8, 128), 1)
    turn = (128 - off) % 128
    seen = jnp.where(lane < 128 - off, pltpu.roll(one, turn, 1), pltpu.roll(two, turn, 1))
    seen = jnp.where(lane < CH, seen, -1000)[:1]
    doc = lax.broadcasted_iota(jnp.int32, (128, 128), 0)
    oh[...] = (doc == seen).astype(F32)
    cnt[...] = nt(jnp.ones((8, 128), F32), (doc - 64 == seen).astype(F32))
    for i in range(ROWS // 128):
        group = ids[pl.ds(i, 1), :]
        every[:, pl.ds(i * 128, 128)] = (doc == group).astype(jnp.bfloat16)
    s2(0)
    q3a.wait_recv()
    q4a = qsend(6, 3, 4, lo, y_up)
    q2b.wait_recv()
    q4b = qsend(7, 2, 4, hi, y_dn)
    q5 = [qsend(10, 2, 5, quarter[0], x_lo), qsend(11, 2, 5, quarter[1], x_lo)]
    q7 = []
    q1a.wait_recv()
    q6a = qsend(8, 1, 6, lo, y_up)
    s3(0)
    q2a.wait_recv()
    q5 += [qsend(12, 2, 5, quarter[2], x_lo), qsend(13, 2, 5, quarter[3], x_lo)]
    q1b.wait_recv()
    q6b = qsend(9, 1, 6, hi, y_up)
    mm(1)
    q3b.wait_recv()
    s1(1)
    s1b(1)
    mm(2, 3, between=lambda: forward(0))
    forward(1)
    s1(2)
    s1b(2)
    s2(1)
    s1(3)
    s1b(3)
    forward(2)
    q4a.wait_recv()
    q4b.wait_recv()
    mm(4, between=lambda: s2(2))
    forward(3)
    s1(4)
    s1b(4)
    s3(1)
    s2(3)
    mm(5, between=lambda: s3(2))
    s1(5)
    s1b(5)
    s2(4)
    s4(0)
    s3(3)
    for cp in (q6a, q6b, *q7):
        cp.wait_recv()
    mm(6, 7, between=lambda: s2(5))
    s1(6)
    s1(7)
    s1b(6)
    s1b(7)
    s4(1)
    s4(2)
    s3(4)
    s4(3)
    s2(6)
    s2(7)
    s3(5)
    s4(4)
    s3(6)
    s4(5)
    s3(7)
    shared_a = share_a()
    s4(6)
    s4(7)
    shared_b = share_b()
    early = finish_a(shared_a)
    late = finish_b(shared_b)
    scores_out[...] = rows_of(6, 8, gathered(gb, 8), scores_out[...])
    mean(early, late)
    for cp in sent:
        cp.wait_send()


def body(activations, deltas, query_in, query_out, doc_ids):
    ids = doc_ids.reshape(ROWS // 128, 128)
    any_ = pl.BlockSpec(memory_space=pl.ANY)
    vmem = pl.BlockSpec(memory_space=pltpu.VMEM)
    dma = pltpu.SemaphoreType.DMA
    scores, docs = pl.pallas_call(
        kernel,
        out_shape=(
            jax.ShapeDtypeStruct((32, ROWS), F32),
            jax.ShapeDtypeStruct((32, 64), F32),
        ),
        in_specs=[any_] * 5,
        out_specs=(vmem, vmem),
        scratch_shapes=[
            pltpu.VMEM((ROWS, KIN), jnp.bfloat16),
            pltpu.VMEM((ROWS, KOUT), jnp.bfloat16),
            pltpu.VMEM((NB, K, 128), jnp.bfloat16),
            pltpu.VMEM((NB, ROWS, 256), F32),
            pltpu.VMEM((NB, HALF, 256), F32),
            pltpu.VMEM((NB, 7, CR, 256), jnp.int16),
            pltpu.VMEM((NB, 7, CR, 256), jnp.int16),
            pltpu.VMEM((NB, CH, 256), F32),
            pltpu.VMEM((NB, 8, 128), F32),
            pltpu.VMEM((8, 128), F32),
            pltpu.VMEM((128, 128), F32),
            pltpu.VMEM((128, ROWS), jnp.bfloat16),
            pltpu.VMEM((ROWS // 128, 128), jnp.int32),
            pltpu.VMEM((24, 128), F32),
            pltpu.VMEM((16, 128), F32),
            pltpu.VMEM((16, 24, 128), F32),
            pltpu.VMEM((16, 16, 128), F32),
            pltpu.VMEM((8, 32, 128), F32),
            pltpu.VMEM((8, 8, 128), F32),
            dma((5,)), dma((18,)), dma((18,)), dma((7, NB)), dma((7, NB)),
            dma((NB, HALF // TM)), dma((NB, HALF // TM)),
            dma((2, 15)), dma((2, 15)), dma((2, 7)), dma((2, 7)),
        ],
        compiler_params=pltpu.CompilerParams(
            collective_id=0, has_side_effects=True, vmem_limit_bytes=60 * 1024 * 1024
        ),
    )(activations, deltas, query_in, query_out, ids)
    def finish(a, b, oa, ob):
        oa[...] = a[...]
        ob[...] = b[...]

    scores, docs = pl.pallas_call(
        finish,
        out_shape=(
            jax.ShapeDtypeStruct((32, ROWS), F32),
            jax.ShapeDtypeStruct((32, 64), F32),
        ),
        in_specs=[vmem, vmem],
        out_specs=(vmem, vmem),
    )(scores, docs)
    return scores.T, docs.T


def solution(mesh):
    return jax.shard_map(
        body,
        mesh=mesh,
        in_specs=(
            P("dp", "tensor"),
            P("dp", "tensor"),
            P("tensor", "dp"),
            P("tensor", "dp"),
            P("dp"),
        ),
        out_specs=(P("dp", None), P()),
        check_vma=False,
    )
```

```python
import jax
import jax.numpy as jnp
from jax import lax
from jax.experimental import pallas as pl
from jax.experimental.pallas import tpu as pltpu
from jax.sharding import PartitionSpec as P

RANK = 32
MESH = pl.DeviceIdType.MESH
F32 = jnp.float32
HIGHEST = lax.Precision.HIGHEST

ROWS = 1536
HALF = ROWS // 2
ZCH = HALF // 4
CH = ZCH // 2
KIN = 512
KOUT = 1792
K = KIN + KOUT
KH = K // 2
NB = 8
TM = 256
HA, HB, RMA, RMB, RPA, RPB, XH = range(7)
KQ = K // 4
GR = 16
CR = CH + 8
UNIT = 32704.0


def nt(a, b):
    return lax.dot_general(
        a, b, (((1,), (1,)), ((), ())), precision=HIGHEST, preferred_element_type=F32
    )


def enc(x):
    codes, tops = [], []
    for i in range(CH // GR):
        part = x[i * GR : (i + 1) * GR]
        top = jnp.maximum(jnp.max(jnp.abs(part), axis=0, keepdims=True), F32(2.0**-110))
        top = jnp.ceil(jnp.log2(top))
        codes.append(jnp.round(part * (jnp.exp2(-top) * F32(UNIT))))
        tops.append(top)
    tops.append(jnp.zeros((8 - CH // GR, x.shape[1]), F32))
    rows = codes + [jnp.concatenate(tops, axis=0)]
    return jnp.concatenate(rows, axis=0).astype(jnp.int32).astype(jnp.int16)


def dec(m):
    tops = m[CH:].astype(jnp.int32).astype(F32)
    tops = jnp.exp2(tops) * F32(1.0 / UNIT)
    out = []
    for i in range(CH // GR):
        part = m[i * GR : (i + 1) * GR].astype(jnp.int32).astype(F32)
        out.append(part * tops[i : i + 1])
    return jnp.concatenate(out, axis=0)


def kernel(
    act, dl, qi, qo, ids_in, scores_hbm, docs_out,
    a_in, a_out, q, p, dbuf, sb, rb, fin, acc, cnt, oh, every, ids, scores_out, msga, msgb, ga, gb, dpa, dpb,
    lsem, ss, qr, rr, mr, gr, dr,
):
    dp = lax.axis_index("dp")
    t = lax.axis_index("tensor")
    xl, y = dp // 4, dp % 4
    hx, z, c = t // 8, (t // 2) % 4, t % 2

    x_lo = {"dp": (dp + 4) % 8, "tensor": t}
    y_up = {"dp": xl * 4 + (y + 1) % 4, "tensor": t}
    y_dn = {"dp": xl * 4 + (y + 3) % 4, "tensor": t}
    x_hi = {"dp": dp, "tensor": (t + 8) % 16}
    z_up = {"dp": dp, "tensor": hx * 8 + ((z + 1) % 4) * 2 + c}
    z_dn = {"dp": dp, "tensor": hx * 8 + ((z + 3) % 4) * 2 + c}
    mate = {"dp": dp, "tensor": hx * 8 + z * 2 + 1 - c}

    loads = [
        pltpu.make_async_copy(qi, q.at[0, pl.ds(0, KIN)], lsem.at[0]),
        pltpu.make_async_copy(qo, q.at[0, pl.ds(KIN, KOUT)], lsem.at[1]),
        pltpu.make_async_copy(act, a_in, lsem.at[2]),
        pltpu.make_async_copy(dl, a_out, lsem.at[3]),
        pltpu.make_async_copy(ids_in, ids, lsem.at[4]),
    ]
    for cp in loads:
        cp.start()

    barrier = pltpu.get_barrier_semaphore()
    near = (x_lo, y_up, y_dn, x_hi, z_up, z_dn, mate)
    for to in near:
        pl.semaphore_signal(barrier, inc=1, device_id=to, device_id_type=MESH)
    pl.semaphore_wait(barrier, len(near))

    def send(src, dst, ssem, rsem, to):
        cp = pltpu.make_async_remote_copy(
            src_ref=src, dst_ref=dst, send_sem=ssem, recv_sem=rsem,
            device_id=to, device_id_type=MESH,
        )
        cp.start()
        return cp

    lo, hi = pl.ds(0, KH), pl.ds(KH, KH)
    quarter = [pl.ds(i * KQ, KQ) for i in (2, 3, 0, 1)]

    def qsend(n, src, dst, rows, to):
        return send(q.at[src, rows], q.at[dst, rows], ss.at[0], qr.at[n], to)

    loads[0].wait()
    loads[1].wait()
    q1a = qsend(0, 0, 1, lo, x_lo)
    q3a = qsend(1, 0, 3, lo, y_up)
    q2b = qsend(2, 0, 2, hi, y_dn)
    q1b = qsend(3, 0, 1, hi, x_lo)
    q3b = qsend(4, 0, 3, hi, y_up)
    q2a = qsend(5, 0, 2, lo, y_dn)

    slot = c * 8 + z * 2 + hx

    moves = {}

    def rsend(b, role, src, dst, to):
        moves[b, role] = send(src, dst, ss.at[1], rr.at[role, b], to)

    own, other = c * HALF, (1 - c) * HALF

    def code(b, role, x, to):
        sb[b, role] = enc(x)
        rsend(b, role, sb.at[b, role], rb.at[b, role], to)

    def chip(b, dz, part):
        rel = ((z + dz) % 4) * ZCH + part * CH
        rows = pl.ds(pl.multiple_of(own + rel, CH), CH)
        return p[b, rows, :] + dbuf[b, pl.ds(pl.multiple_of(rel, CH), CH), :]

    def tile(bs, rows):
        for lhs, first, deep, col in ((a_in, 0, KIN, 0), (a_out, KIN, KOUT, 128)):
            rhs = [q[b, pl.ds(first, deep), :] for b in bs]
            rhs = rhs[0] if len(bs) == 1 else jnp.concatenate(rhs, axis=1)
            out = jnp.dot(lhs[rows, :], rhs, preferred_element_type=F32)
            for i, b in enumerate(bs):
                p[b, rows, pl.ds(col, 128)] = out[:, i * 128 : (i + 1) * 128]

    pieces = HALF // TM

    def piece(b, i, start=False):
        rows = pl.ds(pl.multiple_of(other + i * TM, TM), TM)
        cp = pltpu.make_async_remote_copy(
            src_ref=p.at[b, rows],
            dst_ref=dbuf.at[b, pl.ds(pl.multiple_of(i * TM, TM), TM)],
            send_sem=ss.at[2], recv_sem=mr.at[b, i],
            device_id=mate, device_id_type=MESH,
        )
        if start:
            cp.start()
        return cp

    def mm(*bs, between=lambda: None):
        def first(i, carry):
            tile(bs, pl.ds(pl.multiple_of(other + i * TM, TM), TM))
            for b in bs:
                piece(b, i, True)
            return carry

        def rest(i, carry):
            tile(bs, pl.ds(pl.multiple_of(own + i * TM, TM), TM))
            return carry

        lax.fori_loop(0, pieces, first, 0)
        between()
        lax.fori_loop(0, pieces, rest, 0)
        for b in bs:
            for i in range(pieces):
                moves[b, "core", i] = piece(b, i)

    def s1(b):
        for i in range(pieces):
            moves[b, "core", i].wait_recv()
        code(b, HA, chip(b, 2, 0), z_up)
        code(b, HB, chip(b, 2, 1), z_dn)

    def s1b(b):
        code(b, RMB, chip(b, 1, 1), z_up)
        code(b, RPA, chip(b, 3, 0), z_dn)

    def s2(b):
        moves[b, HA].wait_recv()
        code(b, RMA, chip(b, 1, 0) + dec(rb[b, HA]), z_up)
        moves[b, HB].wait_recv()
        code(b, RPB, chip(b, 3, 1) + dec(rb[b, HB]), z_dn)

    def s3(b):
        for role in (RMB, RPA, RMA, RPB):
            moves[b, role].wait_recv()
        far = 1 - hx
        code(b, XH, chip(b, 0, far) + dec(rb[b, RMA + far]) + dec(rb[b, RPA + far]), x_hi)
        fin[b] = chip(b, 0, hx) + dec(rb[b, RMA + hx]) + dec(rb[b, RPA + hx])

    source = [
        dp, (dp + 4) % 8,
        xl * 4 + (y + 1) % 4, xl * 4 + (y + 3) % 4, xl * 4 + (y + 2) % 4,
        (1 - xl) * 4 + (y + 1) % 4, (1 - xl) * 4 + (y + 3) % 4, (1 - xl) * 4 + (y + 2) % 4,
    ]

    def s4(b):
        moves[b, XH].wait_recv()
        total = fin[b] + dec(rb[b, XH])
        prod = total[:, :128] * total[:, 128:]
        prod = jnp.concatenate([prod, jnp.zeros((128 - CH, 128), F32)], axis=0)
        row = lax.broadcasted_iota(jnp.int32, (8, 128), 0)
        col = lax.broadcasted_iota(jnp.int32, (8, 128), 1)
        pick = jnp.where(row == (b % 2) * 4 + col // RANK, F32(RANK ** -0.5), F32(0))
        acc[b] = nt(pick, prod)

    def every_one(buf, n, ssem, rsem):
        return pltpu.make_async_remote_copy(
            src_ref=buf.at[pl.ds(0, n)], dst_ref=buf.at[pl.ds(0, n)], send_sem=ssem,
            recv_sem=rsem, device_id=mate, device_id_type=MESH,
        )

    def spread(msg, g, n):
        g[slot] = msg[...]
        for k in range(1, 16):
            to = {"dp": dp, "tensor": (t + k) % 16}
            send(msg, g.at[slot], ss.at[3 + n], gr.at[n], to)
        return every_one(g, 15, ss.at[3 + n], gr.at[n])

    def share_a():
        for b in range(0, 6, 2):
            msga[pl.ds(b * 4, 8), :] = acc[b] + acc[b + 1]
        return spread(msga, ga, 0)

    def share_b():
        mine = acc[6] + acc[7]
        msgb[pl.ds(0, 8), :] = mine
        msgb[pl.ds(8, 8), :] = nt(mine, oh[...]) + cnt[...]
        return spread(msgb, gb, 1)

    def rows_of(first, last, found, out, source=source):
        row = lax.broadcasted_iota(jnp.int32, out.shape, 0)
        for b in range(first, last):
            for j in range(4):
                i = (b - first) * 4 + j
                line = jnp.broadcast_to(found[i : i + 1], out.shape)
                out = jnp.where(row == source[b] * 4 + j, line, out)
        return out

    def gathered(g, rows):
        return jnp.concatenate([g[m, pl.ds(0, rows), :][:, :CH] for m in range(16)], axis=1)

    def finish_a(got):
        got.wait_recv()
        found = gathered(ga, 24)
        scores_out[...] = rows_of(0, 6, found, jnp.zeros((32, ROWS), F32))
        one = found.astype(jnp.bfloat16)
        left = found - one.astype(F32)
        two = left.astype(jnp.bfloat16)
        three = (left - two.astype(F32)).astype(jnp.bfloat16)
        sums = jnp.zeros((24, 128), F32)
        for part in (three, two, one):
            sums = sums + lax.dot_general(
                part, every[...], (((1,), (1,)), ((), ())), preferred_element_type=F32
            )
        return across(dpa, rows_of(0, 6, sums, jnp.zeros((32, 128), F32)), 0)

    def finish_b(got):
        got.wait_recv()
        part = gb[0, pl.ds(8, 8), :]
        for m in range(1, 16):
            part = part + gb[m, pl.ds(8, 8), :]
        return across(dpb, part, 1)

    def across(buf, part, n):
        buf[dp] = part
        for k in range(1, 8):
            to = {"dp": (dp + k) % 8, "tensor": t}
            send(buf.at[dp], buf.at[dp], ss.at[5 + n], dr.at[n], to)
        return every_one(buf, 7, ss.at[5 + n], dr.at[n])

    def mean(early, late):
        early.wait_recv()
        whole = dpa[0]
        for m in range(1, 8):
            whole = whole + dpa[m]
        late.wait_recv()
        for m in range(8):
            where = [(1 - m // 4) * 4 + (m + 3) % 4, (1 - m // 4) * 4 + (m + 2) % 4]
            whole = whole + rows_of(0, 2, dpb[m], jnp.zeros((32, 128), F32), where)
        held = dpb[0, pl.ds(0, 1), :]
        for m in range(1, 8):
            held = held + dpb[m, pl.ds(0, 1), :]
        held = jnp.broadcast_to(pltpu.roll(jnp.broadcast_to(held, (8, 128)), 64, 1)[:1], (32, 128))
        docs_out[...] = (whole / held)[:, :64]

    def forward(n):
        q5[n].wait_recv()
        q7.append(qsend(14 + n, 5, 7, quarter[n], y_dn))

    loads[2].wait()
    loads[3].wait()
    mm(0)
    s1(0)
    s1b(0)
    loads[4].wait()
    at = slot * CH
    line, off = at // 128, at % 128
    one = jnp.broadcast_to(ids[pl.ds(line, 1), :], (8, 128))
    two = jnp.broadcast_to(ids[pl.ds(jnp.minimum(line + 1, ROWS // 128 - 1), 1), :], (8, 128))
    lane = lax.broadcasted_iota(jnp.int32, (8, 128), 1)
    turn = (128 - off) % 128
    seen = jnp.where(lane < 128 - off, pltpu.roll(one, turn, 1), pltpu.roll(two, turn, 1))
    seen = jnp.where(lane < CH, seen, -1000)[:1]
    doc = lax.broadcasted_iota(jnp.int32, (128, 128), 0)
    oh[...] = (doc == seen).astype(F32)
    cnt[...] = nt(jnp.ones((8, 128), F32), (doc - 64 == seen).astype(F32))
    for i in range(ROWS // 128):
        group = ids[pl.ds(i, 1), :]
        every[:, pl.ds(i * 128, 128)] = (doc == group).astype(jnp.bfloat16)
    s2(0)
    q3a.wait_recv()
    q4a = qsend(6, 3, 4, lo, y_up)
    q2b.wait_recv()
    q4b = qsend(7, 2, 4, hi, y_dn)
    q5 = [qsend(10, 2, 5, quarter[0], x_lo), qsend(11, 2, 5, quarter[1], x_lo)]
    q7 = []
    q1a.wait_recv()
    q6a = qsend(8, 1, 6, lo, y_up)
    s3(0)
    q2a.wait_recv()
    q5 += [qsend(12, 2, 5, quarter[2], x_lo), qsend(13, 2, 5, quarter[3], x_lo)]
    q1b.wait_recv()
    q6b = qsend(9, 1, 6, hi, y_up)
    mm(1)
    q3b.wait_recv()
    s1(1)
    s1b(1)
    mm(2, 3, between=lambda: forward(0))
    forward(1)
    s1(2)
    s1b(2)
    s2(1)
    s1(3)
    s1b(3)
    forward(2)
    q4a.wait_recv()
    q4b.wait_recv()
    mm(4)
    s2(2)
    forward(3)
    s1(4)
    s1b(4)
    s3(1)
    s2(3)
    mm(5)
    s1(5)
    s1b(5)
    s3(2)
    s2(4)
    for cp in (q6a, q6b, *q7):
        cp.wait_recv()
    mm(6, 7, between=lambda: s2(5))
    s1(6)
    s1(7)
    s1b(6)
    s1b(7)
    s3(3)
    s4(0)
    s4(1)
    s4(2)
    s3(4)
    s4(3)
    s2(6)
    s2(7)
    s3(5)
    s4(4)
    s3(6)
    s4(5)
    s3(7)
    shared_a = share_a()
    s4(6)
    s4(7)
    shared_b = share_b()
    early = finish_a(shared_a)
    late = finish_b(shared_b)
    scores_out[...] = rows_of(6, 8, gathered(gb, 8), scores_out[...])
    out = pltpu.make_async_copy(scores_out, scores_hbm, lsem.at[0])
    out.start()
    mean(early, late)
    every_one(q, 7, ss.at[0], ss.at[0]).wait_send()
    every_one(sb, NB, ss.at[1], ss.at[1]).wait_send()
    every_one(dbuf, NB, ss.at[2], ss.at[2]).wait_send()
    shared_a.wait_send()
    shared_b.wait_send()
    early.wait_send()
    late.wait_send()
    out.wait()


def body(activations, deltas, query_in, query_out, doc_ids):
    ids = doc_ids.reshape(ROWS // 128, 128)
    any_ = pl.BlockSpec(memory_space=pl.ANY)
    vmem = pl.BlockSpec(memory_space=pltpu.VMEM)
    dma = pltpu.SemaphoreType.DMA
    scores, docs = pl.pallas_call(
        kernel,
        out_shape=(
            jax.ShapeDtypeStruct((32, ROWS), F32),
            jax.ShapeDtypeStruct((32, 64), F32),
        ),
        in_specs=[any_] * 5,
        out_specs=(any_, vmem),
        scratch_shapes=[
            pltpu.VMEM((ROWS, KIN), jnp.bfloat16),
            pltpu.VMEM((ROWS, KOUT), jnp.bfloat16),
            pltpu.VMEM((NB, K, 128), jnp.bfloat16),
            pltpu.VMEM((NB, ROWS, 256), F32),
            pltpu.VMEM((NB, HALF, 256), F32),
            pltpu.VMEM((NB, 7, CR, 256), jnp.int16),
            pltpu.VMEM((NB, 7, CR, 256), jnp.int16),
            pltpu.VMEM((NB, CH, 256), F32),
            pltpu.VMEM((NB, 8, 128), F32),
            pltpu.VMEM((8, 128), F32),
            pltpu.VMEM((128, 128), F32),
            pltpu.VMEM((128, ROWS), jnp.bfloat16),
            pltpu.VMEM((ROWS // 128, 128), jnp.int32),
            pltpu.VMEM((32, ROWS), F32),
            pltpu.VMEM((24, 128), F32),
            pltpu.VMEM((16, 128), F32),
            pltpu.VMEM((16, 24, 128), F32),
            pltpu.VMEM((16, 16, 128), F32),
            pltpu.VMEM((8, 32, 128), F32),
            pltpu.VMEM((8, 8, 128), F32),
            dma((5,)), dma((7,)), dma((18,)), dma((7, NB)), dma((NB, HALF // TM)), dma((2,)), dma((2,)),
        ],
        compiler_params=pltpu.CompilerParams(
            collective_id=0, has_side_effects=True, vmem_limit_bytes=60 * 1024 * 1024
        ),
    )(activations, deltas, query_in, query_out, ids)
    def finish(a, b, oa, ob):
        oa[...] = a[...]
        ob[...] = b[...]

    scores, docs = pl.pallas_call(
        finish,
        out_shape=(
            jax.ShapeDtypeStruct((32, ROWS), F32),
            jax.ShapeDtypeStruct((32, 64), F32),
        ),
        in_specs=[vmem, vmem],
        out_specs=(vmem, vmem),
    )(scores, docs)
    return scores.T, docs.T


def solution(mesh):
    return jax.shard_map(
        body,
        mesh=mesh,
        in_specs=(
            P("dp", "tensor"),
            P("dp", "tensor"),
            P("tensor", "dp"),
            P("tensor", "dp"),
            P("dp"),
        ),
        out_specs=(P("dp", None), P()),
        check_vma=False,
    )
```

```python
import jax
import jax.numpy as jnp
from jax import lax
from jax.experimental import pallas as pl
from jax.experimental.pallas import tpu as pltpu
from jax.sharding import PartitionSpec as P

RANK = 32
MESH = pl.DeviceIdType.MESH
F32 = jnp.float32
HIGHEST = lax.Precision.HIGHEST

ROWS = 1536
HALF = ROWS // 2
ZCH = HALF // 4
CH = ZCH // 2
KIN = 512
KOUT = 1792
K = KIN + KOUT
KH = K // 2
NB = 8
TM = HALF // 2
HA, HB, RMA, RMB, RPA, RPB, XH = range(7)
KQ = K // 4
GR = 16
CR = CH + 8
UNIT = 32704.0


def nt(a, b):
    return lax.dot_general(
        a, b, (((1,), (1,)), ((), ())), precision=HIGHEST, preferred_element_type=F32
    )


def enc(x):
    codes, tops = [], []
    for i in range(CH // GR):
        part = x[i * GR : (i + 1) * GR]
        top = jnp.maximum(jnp.max(jnp.abs(part), axis=0, keepdims=True), F32(2.0**-110))
        top = jnp.ceil(jnp.log2(top))
        codes.append(jnp.round(part * (jnp.exp2(-top) * F32(UNIT))))
        tops.append(top)
    tops.append(jnp.zeros((8 - CH // GR, x.shape[1]), F32))
    rows = codes + [jnp.concatenate(tops, axis=0)]
    return jnp.concatenate(rows, axis=0).astype(jnp.int32).astype(jnp.int16)


def dec(m):
    tops = m[CH:].astype(jnp.int32).astype(F32)
    tops = jnp.exp2(tops) * F32(1.0 / UNIT)
    out = []
    for i in range(CH // GR):
        part = m[i * GR : (i + 1) * GR].astype(jnp.int32).astype(F32)
        out.append(part * tops[i : i + 1])
    return jnp.concatenate(out, axis=0)


def kernel(
    act, dl, qi, qo, ids_in, scores_hbm, docs_out,
    a_in, a_out, q, p, dbuf, sb, rb, fin, acc, cnt, oh, every, ids, scores_out, msga, msgb, ga, gb, dpa, dpb,
    lsem, ss, qr, rr, mr, gr, dr,
):
    dp = lax.axis_index("dp")
    t = lax.axis_index("tensor")
    xl, y = dp // 4, dp % 4
    hx, z, c = t // 8, (t // 2) % 4, t % 2

    x_lo = {"dp": (dp + 4) % 8, "tensor": t}
    y_up = {"dp": xl * 4 + (y + 1) % 4, "tensor": t}
    y_dn = {"dp": xl * 4 + (y + 3) % 4, "tensor": t}
    x_hi = {"dp": dp, "tensor": (t + 8) % 16}
    z_up = {"dp": dp, "tensor": hx * 8 + ((z + 1) % 4) * 2 + c}
    z_dn = {"dp": dp, "tensor": hx * 8 + ((z + 3) % 4) * 2 + c}
    mate = {"dp": dp, "tensor": hx * 8 + z * 2 + 1 - c}

    loads = [
        pltpu.make_async_copy(qi, q.at[0, pl.ds(0, KIN)], lsem.at[0]),
        pltpu.make_async_copy(qo, q.at[0, pl.ds(KIN, KOUT)], lsem.at[1]),
        pltpu.make_async_copy(act, a_in, lsem.at[2]),
        pltpu.make_async_copy(dl, a_out, lsem.at[3]),
        pltpu.make_async_copy(ids_in, ids, lsem.at[4]),
    ]
    for cp in loads:
        cp.start()

    barrier = pltpu.get_barrier_semaphore()
    near = (x_lo, y_up, y_dn, x_hi, z_up, z_dn, mate)
    for to in near:
        pl.semaphore_signal(barrier, inc=1, device_id=to, device_id_type=MESH)
    pl.semaphore_wait(barrier, len(near))

    def send(src, dst, ssem, rsem, to):
        cp = pltpu.make_async_remote_copy(
            src_ref=src, dst_ref=dst, send_sem=ssem, recv_sem=rsem,
            device_id=to, device_id_type=MESH,
        )
        cp.start()
        return cp

    lo, hi = pl.ds(0, KH), pl.ds(KH, KH)
    quarter = [pl.ds(i * KQ, KQ) for i in (2, 3, 0, 1)]

    def qsend(n, src, dst, rows, to):
        return send(q.at[src, rows], q.at[dst, rows], ss.at[0], qr.at[n], to)

    loads[0].wait()
    loads[1].wait()
    q1a = qsend(0, 0, 1, lo, x_lo)
    q3a = qsend(1, 0, 3, lo, y_up)
    q2b = qsend(2, 0, 2, hi, y_dn)
    q1b = qsend(3, 0, 1, hi, x_lo)
    q3b = qsend(4, 0, 3, hi, y_up)
    q2a = qsend(5, 0, 2, lo, y_dn)

    slot = c * 8 + z * 2 + hx

    moves = {}

    def rsend(b, role, src, dst, to):
        moves[b, role] = send(src, dst, ss.at[1], rr.at[role, b], to)

    own, other = c * HALF, (1 - c) * HALF

    def code(b, role, x, to):
        sb[b, role] = enc(x)
        rsend(b, role, sb.at[b, role], rb.at[b, role], to)

    def chip(b, dz, part):
        rel = ((z + dz) % 4) * ZCH + part * CH
        rows = pl.ds(pl.multiple_of(own + rel, CH), CH)
        return p[b, rows, :] + dbuf[b, pl.ds(pl.multiple_of(rel, CH), CH), :]

    def tile(bs, rows):
        for lhs, first, deep, col in ((a_in, 0, KIN, 0), (a_out, KIN, KOUT, 128)):
            rhs = [q[b, pl.ds(first, deep), :] for b in bs]
            rhs = rhs[0] if len(bs) == 1 else jnp.concatenate(rhs, axis=1)
            out = jnp.dot(lhs[rows, :], rhs, preferred_element_type=F32)
            for i, b in enumerate(bs):
                p[b, rows, pl.ds(col, 128)] = out[:, i * 128 : (i + 1) * 128]

    pieces = HALF // TM

    def sect(k, base):
        return pl.ds(pl.multiple_of(base + ((z + 2) % 4 // 2 + k) % 2 * TM, TM), TM)

    def piece(b, k, start=False):
        cp = pltpu.make_async_remote_copy(
            src_ref=p.at[b, sect(k, other)], dst_ref=dbuf.at[b, sect(k, 0)],
            send_sem=ss.at[2], recv_sem=mr.at[b, k], device_id=mate, device_id_type=MESH,
        )
        if start:
            cp.start()
        return cp

    def mm(*bs, between=lambda: None):
        def part(k):
            def step(i, carry):
                tile(bs, sect(k, (1 - c + i) % 2 * HALF))

                @pl.when(i == 0)
                def _():
                    for b in bs:
                        piece(b, k, True)

                return carry

            lax.fori_loop(0, 2, step, 0)

        part(0)
        between()
        part(1)

    def met(b, k):
        piece(b, k).wait_recv()

    def s1(b):
        met(b, 0)
        code(b, HA, chip(b, 2, 0), z_up)
        code(b, HB, chip(b, 2, 1), z_dn)

    def s1b(b):
        met(b, 1)
        code(b, RMB, chip(b, 1, 1), z_up)
        code(b, RPA, chip(b, 3, 0), z_dn)

    def s2(b):
        moves[b, HA].wait_recv()
        code(b, RMA, chip(b, 1, 0) + dec(rb[b, HA]), z_up)
        moves[b, HB].wait_recv()
        code(b, RPB, chip(b, 3, 1) + dec(rb[b, HB]), z_dn)

    def s3(b):
        for role in (RMB, RPA, RMA, RPB):
            moves[b, role].wait_recv()
        far = 1 - hx
        code(b, XH, chip(b, 0, far) + dec(rb[b, RMA + far]) + dec(rb[b, RPA + far]), x_hi)
        fin[b] = chip(b, 0, hx) + dec(rb[b, RMA + hx]) + dec(rb[b, RPA + hx])

    source = [
        dp, (dp + 4) % 8,
        xl * 4 + (y + 1) % 4, xl * 4 + (y + 3) % 4, xl * 4 + (y + 2) % 4,
        (1 - xl) * 4 + (y + 1) % 4, (1 - xl) * 4 + (y + 3) % 4, (1 - xl) * 4 + (y + 2) % 4,
    ]

    def s4(b):
        moves[b, XH].wait_recv()
        total = fin[b] + dec(rb[b, XH])
        prod = total[:, :128] * total[:, 128:]
        prod = jnp.concatenate([prod, jnp.zeros((128 - CH, 128), F32)], axis=0)
        row = lax.broadcasted_iota(jnp.int32, (8, 128), 0)
        col = lax.broadcasted_iota(jnp.int32, (8, 128), 1)
        pick = jnp.where(row == (b % 2) * 4 + col // RANK, F32(RANK ** -0.5), F32(0))
        acc[b] = nt(pick, prod)

    def every_one(buf, n, ssem, rsem):
        return pltpu.make_async_remote_copy(
            src_ref=buf.at[pl.ds(0, n)], dst_ref=buf.at[pl.ds(0, n)], send_sem=ssem,
            recv_sem=rsem, device_id=mate, device_id_type=MESH,
        )

    def spread(msg, g, n):
        g[slot] = msg[...]
        for k in range(1, 16):
            to = {"dp": dp, "tensor": (t + k) % 16}
            send(msg, g.at[slot], ss.at[3 + n], gr.at[n], to)
        return every_one(g, 15, ss.at[3 + n], gr.at[n])

    def share_a():
        for b in range(0, 6, 2):
            msga[pl.ds(b * 4, 8), :] = acc[b] + acc[b + 1]
        return spread(msga, ga, 0)

    def share_b():
        mine = acc[6] + acc[7]
        msgb[pl.ds(0, 8), :] = mine
        msgb[pl.ds(8, 8), :] = nt(mine, oh[...]) + cnt[...]
        return spread(msgb, gb, 1)

    def rows_of(first, last, found, out, source=source):
        row = lax.broadcasted_iota(jnp.int32, out.shape, 0)
        for b in range(first, last):
            for j in range(4):
                i = (b - first) * 4 + j
                line = jnp.broadcast_to(found[i : i + 1], out.shape)
                out = jnp.where(row == source[b] * 4 + j, line, out)
        return out

    def gathered(g, rows):
        return jnp.concatenate([g[m, pl.ds(0, rows), :][:, :CH] for m in range(16)], axis=1)

    def finish_a(got):
        got.wait_recv()
        found = gathered(ga, 24)
        scores_out[...] = rows_of(0, 6, found, jnp.zeros((32, ROWS), F32))
        one = found.astype(jnp.bfloat16)
        left = found - one.astype(F32)
        two = left.astype(jnp.bfloat16)
        three = (left - two.astype(F32)).astype(jnp.bfloat16)
        sums = jnp.zeros((24, 128), F32)
        for part in (three, two, one):
            sums = sums + lax.dot_general(
                part, every[...], (((1,), (1,)), ((), ())), preferred_element_type=F32
            )
        return across(dpa, rows_of(0, 6, sums, jnp.zeros((32, 128), F32)), 0)

    def finish_b(got):
        got.wait_recv()
        part = gb[0, pl.ds(8, 8), :]
        for m in range(1, 16):
            part = part + gb[m, pl.ds(8, 8), :]
        return across(dpb, part, 1)

    def across(buf, part, n):
        buf[dp] = part
        for k in range(1, 8):
            to = {"dp": (dp + k) % 8, "tensor": t}
            send(buf.at[dp], buf.at[dp], ss.at[5 + n], dr.at[n], to)
        return every_one(buf, 7, ss.at[5 + n], dr.at[n])

    def mean(early, late):
        early.wait_recv()
        whole = dpa[0]
        for m in range(1, 8):
            whole = whole + dpa[m]
        late.wait_recv()
        for m in range(8):
            where = [(1 - m // 4) * 4 + (m + 3) % 4, (1 - m // 4) * 4 + (m + 2) % 4]
            whole = whole + rows_of(0, 2, dpb[m], jnp.zeros((32, 128), F32), where)
        held = dpb[0, pl.ds(0, 1), :]
        for m in range(1, 8):
            held = held + dpb[m, pl.ds(0, 1), :]
        held = jnp.broadcast_to(pltpu.roll(jnp.broadcast_to(held, (8, 128)), 64, 1)[:1], (32, 128))
        docs_out[...] = (whole / held)[:, :64]

    def forward(n):
        q5[n].wait_recv()
        q7.append(qsend(14 + n, 5, 7, quarter[n], y_dn))

    loads[2].wait()
    loads[3].wait()
    mm(0)
    s1(0)
    s1b(0)
    loads[4].wait()
    at = slot * CH
    line, off = at // 128, at % 128
    one = jnp.broadcast_to(ids[pl.ds(line, 1), :], (8, 128))
    two = jnp.broadcast_to(ids[pl.ds(jnp.minimum(line + 1, ROWS // 128 - 1), 1), :], (8, 128))
    lane = lax.broadcasted_iota(jnp.int32, (8, 128), 1)
    turn = (128 - off) % 128
    seen = jnp.where(lane < 128 - off, pltpu.roll(one, turn, 1), pltpu.roll(two, turn, 1))
    seen = jnp.where(lane < CH, seen, -1000)[:1]
    doc = lax.broadcasted_iota(jnp.int32, (128, 128), 0)
    oh[...] = (doc == seen).astype(F32)
    cnt[...] = nt(jnp.ones((8, 128), F32), (doc - 64 == seen).astype(F32))
    for i in range(ROWS // 128):
        group = ids[pl.ds(i, 1), :]
        every[:, pl.ds(i * 128, 128)] = (doc == group).astype(jnp.bfloat16)
    s2(0)
    q3a.wait_recv()
    q4a = qsend(6, 3, 4, lo, y_up)
    q2b.wait_recv()
    q4b = qsend(7, 2, 4, hi, y_dn)
    q5 = [qsend(10, 2, 5, quarter[0], x_lo), qsend(11, 2, 5, quarter[1], x_lo)]
    q7 = []
    q1a.wait_recv()
    q6a = qsend(8, 1, 6, lo, y_up)
    s3(0)
    q2a.wait_recv()
    q5 += [qsend(12, 2, 5, quarter[2], x_lo), qsend(13, 2, 5, quarter[3], x_lo)]
    q1b.wait_recv()
    q6b = qsend(9, 1, 6, hi, y_up)
    mm(1, between=lambda: s1(1))
    q3b.wait_recv()
    s1b(1)
    mm(2, 3, between=lambda: forward(0))
    forward(1)
    s1(2)
    s1b(2)
    s2(1)
    s1(3)
    s1b(3)
    forward(2)
    q4a.wait_recv()
    q4b.wait_recv()
    mm(4)
    s2(2)
    forward(3)
    s1(4)
    s1b(4)
    s3(1)
    s2(3)
    mm(5, between=lambda: s1(5))
    s1b(5)
    s3(2)
    s2(4)
    for cp in (q6a, q6b, *q7):
        cp.wait_recv()

    def ends():
        s2(5)
        s1(6)
        s1(7)

    mm(6, 7, between=ends)
    s1b(6)
    s1b(7)
    s3(3)
    s4(0)
    s4(1)
    s4(2)
    s3(4)
    s2(6)
    s2(7)
    s3(5)
    s4(3)
    s4(4)
    s3(6)
    s4(5)
    s3(7)
    shared_a = share_a()
    s4(6)
    s4(7)
    shared_b = share_b()
    early = finish_a(shared_a)
    late = finish_b(shared_b)
    scores_out[...] = rows_of(6, 8, gathered(gb, 8), scores_out[...])
    out = pltpu.make_async_copy(scores_out, scores_hbm, lsem.at[0])
    out.start()
    mean(early, late)
    every_one(q, 7, ss.at[0], ss.at[0]).wait_send()
    every_one(sb, NB, ss.at[1], ss.at[1]).wait_send()
    every_one(dbuf, NB, ss.at[2], ss.at[2]).wait_send()
    shared_a.wait_send()
    shared_b.wait_send()
    early.wait_send()
    late.wait_send()
    out.wait()


def body(activations, deltas, query_in, query_out, doc_ids):
    ids = doc_ids.reshape(ROWS // 128, 128)
    any_ = pl.BlockSpec(memory_space=pl.ANY)
    vmem = pl.BlockSpec(memory_space=pltpu.VMEM)
    dma = pltpu.SemaphoreType.DMA
    scores, docs = pl.pallas_call(
        kernel,
        out_shape=(
            jax.ShapeDtypeStruct((32, ROWS), F32),
            jax.ShapeDtypeStruct((32, 64), F32),
        ),
        in_specs=[any_] * 5,
        out_specs=(any_, vmem),
        scratch_shapes=[
            pltpu.VMEM((ROWS, KIN), jnp.bfloat16),
            pltpu.VMEM((ROWS, KOUT), jnp.bfloat16),
            pltpu.VMEM((NB, K, 128), jnp.bfloat16),
            pltpu.VMEM((NB, ROWS, 256), F32),
            pltpu.VMEM((NB, HALF, 256), F32),
            pltpu.VMEM((NB, 7, CR, 256), jnp.int16),
            pltpu.VMEM((NB, 7, CR, 256), jnp.int16),
            pltpu.VMEM((NB, CH, 256), F32),
            pltpu.VMEM((NB, 8, 128), F32),
            pltpu.VMEM((8, 128), F32),
            pltpu.VMEM((128, 128), F32),
            pltpu.VMEM((128, ROWS), jnp.bfloat16),
            pltpu.VMEM((ROWS // 128, 128), jnp.int32),
            pltpu.VMEM((32, ROWS), F32),
            pltpu.VMEM((24, 128), F32),
            pltpu.VMEM((16, 128), F32),
            pltpu.VMEM((16, 24, 128), F32),
            pltpu.VMEM((16, 16, 128), F32),
            pltpu.VMEM((8, 32, 128), F32),
            pltpu.VMEM((8, 8, 128), F32),
            dma((5,)), dma((7,)), dma((18,)), dma((7, NB)), dma((NB, HALF // TM)), dma((2,)), dma((2,)),
        ],
        compiler_params=pltpu.CompilerParams(
            collective_id=0, has_side_effects=True, vmem_limit_bytes=60 * 1024 * 1024
        ),
    )(activations, deltas, query_in, query_out, ids)
    def finish(a, b, oa, ob):
        oa[...] = a[...]
        ob[...] = b[...]

    scores, docs = pl.pallas_call(
        finish,
        out_shape=(
            jax.ShapeDtypeStruct((32, ROWS), F32),
            jax.ShapeDtypeStruct((32, 64), F32),
        ),
        in_specs=[vmem, vmem],
        out_specs=(vmem, vmem),
    )(scores, docs)
    return scores.T, docs.T


def solution(mesh):
    return jax.shard_map(
        body,
        mesh=mesh,
        in_specs=(
            P("dp", "tensor"),
            P("dp", "tensor"),
            P("tensor", "dp"),
            P("tensor", "dp"),
            P("dp"),
        ),
        out_specs=(P("dp", None), P()),
        check_vma=False,
    )
```

```python
import jax
import jax.numpy as jnp
from jax import lax
from jax.experimental import pallas as pl
from jax.experimental.pallas import tpu as pltpu
from jax.sharding import PartitionSpec as P

RANK = 32
MESH = pl.DeviceIdType.MESH
F32 = jnp.float32
HIGHEST = lax.Precision.HIGHEST

ROWS = 1536
HALF = ROWS // 2
ZCH = HALF // 4
CH = ZCH // 2
KIN = 512
KOUT = 1792
K = KIN + KOUT
KH = K // 2
NB = 8
TM = HALF // 2
HA, HB, RMA, RMB, RPA, RPB, XH = range(7)
KQ = K // 4
GR = 16
CR = CH + 8
UNIT = 32704.0


def nt(a, b):
    return lax.dot_general(
        a, b, (((1,), (1,)), ((), ())), precision=HIGHEST, preferred_element_type=F32
    )


def enc(x):
    codes, tops = [], []
    for i in range(CH // GR):
        part = x[i * GR : (i + 1) * GR]
        top = jnp.maximum(jnp.max(jnp.abs(part), axis=0, keepdims=True), F32(2.0**-110))
        top = jnp.ceil(jnp.log2(top))
        codes.append(jnp.round(part * (jnp.exp2(-top) * F32(UNIT))))
        tops.append(top)
    tops.append(jnp.zeros((8 - CH // GR, x.shape[1]), F32))
    rows = codes + [jnp.concatenate(tops, axis=0)]
    return jnp.concatenate(rows, axis=0).astype(jnp.int32).astype(jnp.int16)


def dec(m):
    tops = m[CH:].astype(jnp.int32).astype(F32)
    tops = jnp.exp2(tops) * F32(1.0 / UNIT)
    out = []
    for i in range(CH // GR):
        part = m[i * GR : (i + 1) * GR].astype(jnp.int32).astype(F32)
        out.append(part * tops[i : i + 1])
    return jnp.concatenate(out, axis=0)


def kernel(
    act, dl, qi, qo, ids_in, scores_hbm, docs_out,
    a_in, a_out, q, p, dbuf, sb, rb, fin, acc, cnt, oh, every, ids, scores_out, msga, msgb, ga, gb, dpa, dpb,
    lsem, ss, qr, rr, mr, gr, dr,
):
    dp = lax.axis_index("dp")
    t = lax.axis_index("tensor")
    xl, y = dp // 4, dp % 4
    hx, z, c = t // 8, (t // 2) % 4, t % 2

    x_lo = {"dp": (dp + 4) % 8, "tensor": t}
    y_up = {"dp": xl * 4 + (y + 1) % 4, "tensor": t}
    y_dn = {"dp": xl * 4 + (y + 3) % 4, "tensor": t}
    x_hi = {"dp": dp, "tensor": (t + 8) % 16}
    z_up = {"dp": dp, "tensor": hx * 8 + ((z + 1) % 4) * 2 + c}
    z_dn = {"dp": dp, "tensor": hx * 8 + ((z + 3) % 4) * 2 + c}
    mate = {"dp": dp, "tensor": hx * 8 + z * 2 + 1 - c}

    loads = [
        pltpu.make_async_copy(qi, q.at[0, pl.ds(0, KIN)], lsem.at[0]),
        pltpu.make_async_copy(qo, q.at[0, pl.ds(KIN, KOUT)], lsem.at[1]),
        pltpu.make_async_copy(act, a_in, lsem.at[2]),
        pltpu.make_async_copy(dl, a_out, lsem.at[3]),
        pltpu.make_async_copy(ids_in, ids, lsem.at[4]),
    ]
    for cp in loads:
        cp.start()

    barrier = pltpu.get_barrier_semaphore()
    near = (x_lo, y_up, y_dn, x_hi, z_up, z_dn, mate)
    for to in near:
        pl.semaphore_signal(barrier, inc=1, device_id=to, device_id_type=MESH)
    pl.semaphore_wait(barrier, len(near))

    def send(src, dst, ssem, rsem, to):
        cp = pltpu.make_async_remote_copy(
            src_ref=src, dst_ref=dst, send_sem=ssem, recv_sem=rsem,
            device_id=to, device_id_type=MESH,
        )
        cp.start()
        return cp

    lo, hi = pl.ds(0, KH), pl.ds(KH, KH)
    quarter = [pl.ds(i * KQ, KQ) for i in (2, 3, 0, 1)]

    def qsend(n, src, dst, rows, to):
        return send(q.at[src, rows], q.at[dst, rows], ss.at[0], qr.at[n], to)

    loads[0].wait()
    loads[1].wait()
    q1a = qsend(0, 0, 1, lo, x_lo)
    q3a = qsend(1, 0, 3, lo, y_up)
    q2b = qsend(2, 0, 2, hi, y_dn)
    q1b = qsend(3, 0, 1, hi, x_lo)
    q3b = qsend(4, 0, 3, hi, y_up)
    q2a = qsend(5, 0, 2, lo, y_dn)

    slot = c * 8 + z * 2 + hx

    moves = {}

    def rsend(b, role, src, dst, to):
        moves[b, role] = send(src, dst, ss.at[1], rr.at[role, b], to)

    own, other = c * HALF, (1 - c) * HALF

    def code(b, role, x, to):
        sb[b, role] = enc(x)
        rsend(b, role, sb.at[b, role], rb.at[b, role], to)

    def chip(b, dz, part):
        rel = ((z + dz) % 4) * ZCH + part * CH
        rows = pl.ds(pl.multiple_of(own + rel, CH), CH)
        return p[b, rows, :] + dbuf[b, pl.ds(pl.multiple_of(rel, CH), CH), :]

    def tile(bs, rows):
        for lhs, first, deep, col in ((a_in, 0, KIN, 0), (a_out, KIN, KOUT, 128)):
            rhs = [q[b, pl.ds(first, deep), :] for b in bs]
            rhs = rhs[0] if len(bs) == 1 else jnp.concatenate(rhs, axis=1)
            out = jnp.dot(lhs[rows, :], rhs, preferred_element_type=F32)
            for i, b in enumerate(bs):
                p[b, rows, pl.ds(col, 128)] = out[:, i * 128 : (i + 1) * 128]

    pieces = HALF // TM

    def sect(k, base):
        return pl.ds(pl.multiple_of(base + ((z + 2) % 4 // 2 + k) % 2 * TM, TM), TM)

    def piece(b, k, start=False):
        cp = pltpu.make_async_remote_copy(
            src_ref=p.at[b, sect(k, other)], dst_ref=dbuf.at[b, sect(k, 0)],
            send_sem=ss.at[2], recv_sem=mr.at[b, k], device_id=mate, device_id_type=MESH,
        )
        if start:
            cp.start()
        return cp

    def mm(*bs, between=lambda: None):
        def part(k):
            def step(i, carry):
                tile(bs, sect(k, (1 - c + i) % 2 * HALF))

                @pl.when(i == 0)
                def _():
                    for b in bs:
                        piece(b, k, True)

                return carry

            lax.fori_loop(0, 2, step, 0)

        part(0)
        between()
        part(1)

    def met(b, k):
        piece(b, k).wait_recv()

    def s1(b):
        met(b, 0)
        code(b, HA, chip(b, 2, 0), z_up)
        code(b, HB, chip(b, 2, 1), z_dn)

    def s1b(b):
        met(b, 1)
        code(b, RMB, chip(b, 1, 1), z_up)
        code(b, RPA, chip(b, 3, 0), z_dn)

    def s2(b):
        moves[b, HA].wait_recv()
        code(b, RMA, chip(b, 1, 0) + dec(rb[b, HA]), z_up)
        moves[b, HB].wait_recv()
        code(b, RPB, chip(b, 3, 1) + dec(rb[b, HB]), z_dn)

    def s3(b):
        for role in (RMB, RPA, RMA, RPB):
            moves[b, role].wait_recv()
        far = 1 - hx
        code(b, XH, chip(b, 0, far) + dec(rb[b, RMA + far]) + dec(rb[b, RPA + far]), x_hi)
        fin[b] = chip(b, 0, hx) + dec(rb[b, RMA + hx]) + dec(rb[b, RPA + hx])

    source = [
        dp, (dp + 4) % 8,
        xl * 4 + (y + 1) % 4, xl * 4 + (y + 3) % 4, xl * 4 + (y + 2) % 4,
        (1 - xl) * 4 + (y + 1) % 4, (1 - xl) * 4 + (y + 3) % 4, (1 - xl) * 4 + (y + 2) % 4,
    ]

    def s4(b):
        moves[b, XH].wait_recv()
        total = fin[b] + dec(rb[b, XH])
        prod = total[:, :128] * total[:, 128:]
        prod = jnp.concatenate([prod, jnp.zeros((128 - CH, 128), F32)], axis=0)
        row = lax.broadcasted_iota(jnp.int32, (8, 128), 0)
        col = lax.broadcasted_iota(jnp.int32, (8, 128), 1)
        pick = jnp.where(row == (b % 2) * 4 + col // RANK, F32(RANK ** -0.5), F32(0))
        acc[b] = nt(pick, prod)

    def every_one(buf, n, ssem, rsem):
        return pltpu.make_async_remote_copy(
            src_ref=buf.at[pl.ds(0, n)], dst_ref=buf.at[pl.ds(0, n)], send_sem=ssem,
            recv_sem=rsem, device_id=mate, device_id_type=MESH,
        )

    def spread(msg, g, n):
        g[slot] = msg[...]
        for k in range(1, 16):
            to = {"dp": dp, "tensor": (t + k) % 16}
            send(msg, g.at[slot], ss.at[3 + n], gr.at[n], to)
        return every_one(g, 15, ss.at[3 + n], gr.at[n])

    def share_a():
        for b in range(0, 6, 2):
            msga[pl.ds(b * 4, 8), :] = acc[b] + acc[b + 1]
        return spread(msga, ga, 0)

    def share_b():
        mine = acc[6] + acc[7]
        msgb[pl.ds(0, 8), :] = mine
        msgb[pl.ds(8, 8), :] = nt(mine, oh[...]) + cnt[...]
        return spread(msgb, gb, 1)

    def rows_of(first, last, found, out, source=source):
        row = lax.broadcasted_iota(jnp.int32, out.shape, 0)
        for b in range(first, last):
            for j in range(4):
                i = (b - first) * 4 + j
                line = jnp.broadcast_to(found[i : i + 1], out.shape)
                out = jnp.where(row == source[b] * 4 + j, line, out)
        return out

    def gathered(g, rows):
        return jnp.concatenate([g[m, pl.ds(0, rows), :][:, :CH] for m in range(16)], axis=1)

    def finish_a(got):
        got.wait_recv()
        found = gathered(ga, 24)
        scores_out[...] = rows_of(0, 6, found, jnp.zeros((32, ROWS), F32))
        one = found.astype(jnp.bfloat16)
        left = found - one.astype(F32)
        two = left.astype(jnp.bfloat16)
        three = (left - two.astype(F32)).astype(jnp.bfloat16)
        sums = jnp.zeros((24, 128), F32)
        for part in (three, two, one):
            sums = sums + lax.dot_general(
                part, every[...], (((1,), (1,)), ((), ())), preferred_element_type=F32
            )
        return across(dpa, rows_of(0, 6, sums, jnp.zeros((32, 128), F32)), 0)

    def finish_b(got):
        got.wait_recv()
        part = gb[0, pl.ds(8, 8), :]
        for m in range(1, 16):
            part = part + gb[m, pl.ds(8, 8), :]
        return across(dpb, part, 1)

    def across(buf, part, n):
        buf[dp] = part
        for k in range(1, 8):
            to = {"dp": (dp + k) % 8, "tensor": t}
            send(buf.at[dp], buf.at[dp], ss.at[5 + n], dr.at[n], to)
        return every_one(buf, 7, ss.at[5 + n], dr.at[n])

    def mean(early, late):
        early.wait_recv()
        whole = dpa[0]
        for m in range(1, 8):
            whole = whole + dpa[m]
        late.wait_recv()
        for m in range(8):
            where = [(1 - m // 4) * 4 + (m + 3) % 4, (1 - m // 4) * 4 + (m + 2) % 4]
            whole = whole + rows_of(0, 2, dpb[m], jnp.zeros((32, 128), F32), where)
        held = dpb[0, pl.ds(0, 1), :]
        for m in range(1, 8):
            held = held + dpb[m, pl.ds(0, 1), :]
        held = jnp.broadcast_to(pltpu.roll(jnp.broadcast_to(held, (8, 128)), 64, 1)[:1], (32, 128))
        docs_out[...] = (whole / held)[:, :64]

    def forward(n):
        q5[n].wait_recv()
        q7.append(qsend(14 + n, 5, 7, quarter[n], y_dn))

    loads[2].wait()
    loads[3].wait()
    mm(0)
    s1(0)
    s1b(0)
    loads[4].wait()
    at = slot * CH
    line, off = at // 128, at % 128
    one = jnp.broadcast_to(ids[pl.ds(line, 1), :], (8, 128))
    two = jnp.broadcast_to(ids[pl.ds(jnp.minimum(line + 1, ROWS // 128 - 1), 1), :], (8, 128))
    lane = lax.broadcasted_iota(jnp.int32, (8, 128), 1)
    turn = (128 - off) % 128
    seen = jnp.where(lane < 128 - off, pltpu.roll(one, turn, 1), pltpu.roll(two, turn, 1))
    seen = jnp.where(lane < CH, seen, -1000)[:1]
    doc = lax.broadcasted_iota(jnp.int32, (128, 128), 0)
    oh[...] = (doc == seen).astype(F32)
    cnt[...] = nt(jnp.ones((8, 128), F32), (doc - 64 == seen).astype(F32))
    for i in range(ROWS // 128):
        group = ids[pl.ds(i, 1), :]
        every[:, pl.ds(i * 128, 128)] = (doc == group).astype(jnp.bfloat16)
    s2(0)
    q3a.wait_recv()
    q4a = qsend(6, 3, 4, lo, y_up)
    q2b.wait_recv()
    q4b = qsend(7, 2, 4, hi, y_dn)
    q5 = [qsend(10, 2, 5, quarter[0], x_lo), qsend(11, 2, 5, quarter[1], x_lo)]
    q7 = []
    q1a.wait_recv()
    q6a = qsend(8, 1, 6, lo, y_up)
    s3(0)
    q2a.wait_recv()
    q5 += [qsend(12, 2, 5, quarter[2], x_lo), qsend(13, 2, 5, quarter[3], x_lo)]
    q1b.wait_recv()
    q6b = qsend(9, 1, 6, hi, y_up)
    mm(1, between=lambda: s1(1))
    q3b.wait_recv()
    s1b(1)
    mm(2, 3, between=lambda: forward(0))
    forward(1)
    s1(2)
    s1b(2)
    s2(1)
    s1(3)
    s1b(3)
    forward(2)
    q4a.wait_recv()
    q4b.wait_recv()
    mm(4)
    s2(2)
    forward(3)
    s1(4)
    s1b(4)
    s3(1)
    s2(3)
    mm(5, between=lambda: s1(5))
    s1b(5)
    s3(2)
    s2(4)
    for cp in (q6a, q6b, *q7):
        cp.wait_recv()

    def ends():
        s2(5)
        s1(6)
        s1(7)

    mm(6, 7, between=ends)
    s1b(6)
    s1b(7)
    s3(3)
    s4(0)
    s4(1)
    s4(2)
    s3(4)
    s2(6)
    s2(7)
    s3(5)
    s4(3)
    s4(4)
    s3(6)
    s3(7)
    s4(5)
    shared_a = share_a()
    s4(6)
    s4(7)
    shared_b = share_b()
    early = finish_a(shared_a)
    late = finish_b(shared_b)
    scores_out[...] = rows_of(6, 8, gathered(gb, 8), scores_out[...])
    out = pltpu.make_async_copy(scores_out, scores_hbm, lsem.at[0])
    out.start()
    mean(early, late)
    every_one(q, 7, ss.at[0], ss.at[0]).wait_send()
    every_one(sb, NB, ss.at[1], ss.at[1]).wait_send()
    every_one(dbuf, NB, ss.at[2], ss.at[2]).wait_send()
    shared_a.wait_send()
    shared_b.wait_send()
    early.wait_send()
    late.wait_send()
    out.wait()


def body(activations, deltas, query_in, query_out, doc_ids):
    ids = doc_ids.reshape(ROWS // 128, 128)
    any_ = pl.BlockSpec(memory_space=pl.ANY)
    vmem = pl.BlockSpec(memory_space=pltpu.VMEM)
    dma = pltpu.SemaphoreType.DMA
    scores, docs = pl.pallas_call(
        kernel,
        out_shape=(
            jax.ShapeDtypeStruct((32, ROWS), F32),
            jax.ShapeDtypeStruct((32, 64), F32),
        ),
        in_specs=[any_] * 5,
        out_specs=(any_, vmem),
        scratch_shapes=[
            pltpu.VMEM((ROWS, KIN), jnp.bfloat16),
            pltpu.VMEM((ROWS, KOUT), jnp.bfloat16),
            pltpu.VMEM((NB, K, 128), jnp.bfloat16),
            pltpu.VMEM((NB, ROWS, 256), F32),
            pltpu.VMEM((NB, HALF, 256), F32),
            pltpu.VMEM((NB, 7, CR, 256), jnp.int16),
            pltpu.VMEM((NB, 7, CR, 256), jnp.int16),
            pltpu.VMEM((NB, CH, 256), F32),
            pltpu.VMEM((NB, 8, 128), F32),
            pltpu.VMEM((8, 128), F32),
            pltpu.VMEM((128, 128), F32),
            pltpu.VMEM((128, ROWS), jnp.bfloat16),
            pltpu.VMEM((ROWS // 128, 128), jnp.int32),
            pltpu.VMEM((32, ROWS), F32),
            pltpu.VMEM((24, 128), F32),
            pltpu.VMEM((16, 128), F32),
            pltpu.VMEM((16, 24, 128), F32),
            pltpu.VMEM((16, 16, 128), F32),
            pltpu.VMEM((8, 32, 128), F32),
            pltpu.VMEM((8, 8, 128), F32),
            dma((5,)), dma((7,)), dma((18,)), dma((7, NB)), dma((NB, HALF // TM)), dma((2,)), dma((2,)),
        ],
        compiler_params=pltpu.CompilerParams(
            collective_id=0, has_side_effects=True, vmem_limit_bytes=60 * 1024 * 1024
        ),
    )(activations, deltas, query_in, query_out, ids)
    def finish(a, b, oa, ob):
        oa[...] = a[...]
        ob[...] = b[...]

    scores, docs = pl.pallas_call(
        finish,
        out_shape=(
            jax.ShapeDtypeStruct((32, ROWS), F32),
            jax.ShapeDtypeStruct((32, 64), F32),
        ),
        in_specs=[vmem, vmem],
        out_specs=(vmem, vmem),
    )(scores, docs)
    return scores.T, docs.T


def solution(mesh):
    return jax.shard_map(
        body,
        mesh=mesh,
        in_specs=(
            P("dp", "tensor"),
            P("dp", "tensor"),
            P("tensor", "dp"),
            P("tensor", "dp"),
            P("dp"),
        ),
        out_specs=(P("dp", None), P()),
        check_vma=False,
    )
```
